32 devices in a mesh: groups: 2 (over x), ep: 8 (over z, y), node: 2 (over core).
Axes of the slice: x: 2, y: 2, z: 4, core: 2. Of those that a mesh axis runs over, the one named last changes fastest.
Arguments:
- tokens: bfloat16 [1024, 7168], P(('groups', 'ep', 'node')), parts along dimension 0, may hold values from -6 to 6
- expert_ids: int32 [1024, 8], P(('groups', 'ep', 'node')), parts along dimension 0, may hold values from 0 to 15, all different within a row; in each aligned block of 32 rows (0 to 31, 32 to 63, ...) at most 32 rows name the same one
- gate_weights: float32 [1024, 8], P(('groups', 'ep', 'node')), parts along dimension 0, may hold values from 0.05 to 0.5
- gate_up_weight: bfloat16 [16, 7168, 512], P(('ep', 'node')), may hold values from -0.0625 to 0.0625
- down_weight: bfloat16 [16, 256, 7168], P(('ep', 'node')), may hold values from -0.375 to 0.375
Outputs:
- moe_out: bfloat16 [1024, 7168], P(('groups', 'ep', 'node')), parts along dimension 0
The draws below stay inside these ranges and needn't reach their ends.
There are 2 independent parts, one for each index of `groups`. The reference program is written for one: setup_inputs(seed, part) draws one part's arguments, and reference() takes and returns one part's arrays. A program takes and returns all parts, laid end to end along the dimension named above; an argument that names none is the same for every part. Nothing has to cross between parts.
Inputs may be any that keep to these rules, and one draw needn't show every extreme that they name: `expert_ids`: each token names 8 different experts; among the 32 tokens of one device no expert is named by more than 32 of them, a bound that some block reaches.
All inputs are finite; a program needn't handle non-finite values.
Results may differ from the reference program's by a relative error of at most 0.0058.
Values may be sent and summed in bfloat16 or wider, within the bound.
A program may use at most 128 MiB of HBM per device.

```python
import math
import jax
import jax.numpy as jnp
import numpy as np
from jax import lax

D = 7168
TOP = 8
EXP_HID = 256
TOK_DEV = 32
EXPERTS = 16
CAP = 32
TOKENS = 512
N_EP = 8
N_NODE = 2


def level_of(rng, dims, split, smallest, high):
    level = 1.0
    for axis_at, blocks in split:
        heights = jax.random.uniform(jax.random.fold_in(jax.random.fold_in(rng, 6), axis_at), (blocks,), jnp.float32, smallest / len(split), high / len(split))
        level = level * jnp.repeat(jnp.exp(heights), dims[axis_at] // blocks).reshape((-1,) + (1,) * (len(dims) - 1 - axis_at))
    return level


def assign_block(rng, own, number, rows, count, top, most, slope):
    sequence = jax.random.permutation(rng, count)
    heavy_load, common = load_shares(count, rows * top, most, slope, True), load_shares(count, rows * top, most, slope, False)
    places = jnp.arange(count)

    def named(sizes, turn):
        used = int((sizes > 0).sum())
        fixed = max(1, used // 4)
        shifted = fixed + (places - fixed + turn * (used - fixed)) % max(1, count - fixed)
        return jnp.zeros((count,), jnp.int32).at[sequence[jnp.where(places < fixed, places, shifted)]].set(jnp.asarray(sizes, jnp.int32))

    sizes = jnp.where(number % 4 == 0, named(heavy_load, number // 4), named(common, number - number // 4 - 1))
    mixed = jax.random.permutation(jax.random.fold_in(own, 3), count)
    source_of, taker = mixed[0:count // 2 * 2:2], mixed[1:count // 2 * 2:2]
    room = jnp.minimum(sizes[source_of] - 1, most - sizes[taker]) // 2
    room = jnp.where((source_of == sequence[0]) | (taker == sequence[0]) | (sizes[taker] == 0), 0, jnp.maximum(room, 0))
    shifted = jax.random.randint(jax.random.fold_in(own, 4), (count // 2,), 0, 1 << 20) % (room + 1)
    sizes = sizes.at[source_of].add(-shifted).at[taker].add(shifted)
    members = jnp.searchsorted(jnp.cumsum(sizes), jnp.arange(rows * top), side="right").astype(jnp.int32)
    table = members.reshape(top, rows).T
    table = table[jax.random.permutation(jax.random.fold_in(own, 1), rows)]
    turn = jax.random.randint(jax.random.fold_in(own, 2), (rows, 1), 0, top)
    return jnp.take_along_axis(table, (jnp.arange(top)[None, :] + turn) % top, axis=1)


def load_shares(amount, total, reach, skew, full):
    weights = [(1 << 20) // math.isqrt(grade ** skew) + 1 for grade in range(1, amount + 1)]
    largest = reach if full else min(reach, max(-(-total // amount), total * weights[0] // sum(weights)))
    least = 1 if total - largest >= amount - 1 else 0
    given, rest = [largest] + [least] * (amount - 1), total - largest - least * (amount - 1)
    while rest > 0:
        free = [i for i in range(1, amount) if given[i] < largest] or [i for i in range(1, amount) if given[i] < reach]
        pool, left = sum([weights[i] for i in free]), rest
        for i in free:
            extra = min(reach - given[i], max(1, left * weights[i] // pool), rest)
            given[i] = given[i] + extra
            rest = rest - extra
    return np.array(given)


def normal_values(key, extent, spread, reach, cuts=(), held_as=jnp.bfloat16):
    drawn = spread * jax.random.normal(key, extent, jnp.float32)
    if cuts:
        drawn = drawn * level_of(key, extent, cuts, -0.22, 0.18)
    return jnp.clip(drawn, -reach, reach).astype(held_as)


def setup_inputs(seed: int = 0, part: int = 0) -> dict:
    splits = jax.random.split(jax.random.key(seed), 6)
    part_keys = jax.random.split(jax.random.fold_in(splits[5], part), 6)
    tokens = normal_values(part_keys[0], (TOKENS, D), 1.0, 6.0, ((0, 16),))
    expert_ids_keys = jax.random.split(jax.random.fold_in(part_keys[1], 1), TOKENS // TOK_DEV)
    expert_ids_turns = jax.random.permutation(jax.random.fold_in(part_keys[1], 3), TOKENS // TOK_DEV)
    expert_ids = jax.vmap(lambda own, number: assign_block(jax.random.fold_in(part_keys[1], 2), own, number, TOK_DEV, EXPERTS, TOP, CAP, 2))(expert_ids_keys, expert_ids_turns).reshape((TOKENS, TOP))
    gate_weights = jnp.clip(jnp.exp(math.log(0.5) - 2.3025851 * jax.random.uniform(part_keys[2], (TOKENS, TOP), jnp.float32) ** level_of(part_keys[2], (TOKENS, TOP), ((0, 16),), -0.2, 0.2)), 0.05, 0.5)
    gate_up_weight = normal_values(splits[3], (EXPERTS, D, 2 * EXP_HID), D ** -0.5, 0.0625, ((0, 16),))
    down_weight = normal_values(splits[4], (EXPERTS, EXP_HID, D), EXP_HID ** -0.5, 0.375, ((0, 16),))
    return {"tokens": tokens, "expert_ids": expert_ids, "gate_weights": gate_weights, "gate_up_weight": gate_up_weight, "down_weight": down_weight}


def reference(tokens, expert_ids, gate_weights, gate_up_weight, down_weight):
    slot_total = N_EP * N_NODE * CAP
    token_index = jnp.arange(TOKENS, dtype=jnp.int32)

    def per_expert(running, expert):
        chosen = expert_ids == expert
        routed = jnp.any(chosen, axis=1)
        picked = jnp.sum(jnp.where(chosen, gate_weights, jnp.zeros_like(gate_weights)), axis=1)
        position = jnp.cumsum(routed.astype(jnp.int32)) - 1
        where_to = jnp.where(routed, position, slot_total).astype(jnp.int32)
        row_index = jnp.zeros((slot_total,), jnp.int32).at[where_to].set(token_index, mode="drop")
        filled = jnp.zeros((slot_total,), jnp.float32).at[where_to].set(jnp.ones((TOKENS,), jnp.float32), mode="drop")
        gathered = tokens[row_index]
        gate_up = jnp.dot(gathered, gate_up_weight[expert], preferred_element_type=jnp.float32)
        hidden = (jax.nn.silu(gate_up[:, :EXP_HID]) * gate_up[:, EXP_HID:]).astype(jnp.bfloat16)
        result = jnp.dot(hidden, down_weight[expert], preferred_element_type=jnp.float32).astype(jnp.bfloat16)
        weight_row = filled * picked[row_index]
        running = running.at[row_index].add(weight_row[:, None] * result.astype(jnp.float32))
        return running, None

    start = jnp.zeros((TOKENS, D), jnp.float32)
    summed, unused = lax.scan(per_expert, start, jnp.arange(EXPERTS, dtype=jnp.int32))
    return summed.astype(jnp.bfloat16)
```

```python
import functools

import jax
import jax.numpy as jnp
from jax import lax
from jax.experimental import pallas as pl
from jax.experimental.pallas import tpu as pltpu
from jax.sharding import PartitionSpec as P

AXES = ("ep", "node")
DRAIN_AFTER = 8.0


def spread_out(tokens, expert_ids, gate_weights, gate_up_weight, down_weight):
    local_count, inner_width = down_weight.shape[0], down_weight.shape[1]
    device = lax.axis_index("ep") * lax.axis_size("node") + lax.axis_index("node")
    all_tokens = lax.all_gather(tokens, AXES, axis=0, tiled=True)
    all_ids = lax.all_gather(expert_ids, AXES, axis=0, tiled=True)
    all_weights = lax.all_gather(gate_weights, AXES, axis=0, tiled=True)
    total = 0.0
    for local in range(local_count):
        expert = device * local_count + local
        share = jnp.sum(jnp.where(all_ids == expert, all_weights, 0.0), axis=1)
        gate_up = jnp.dot(all_tokens, gate_up_weight[local], preferred_element_type=jnp.float32)
        hidden = (jax.nn.silu(gate_up[:, :inner_width]) * gate_up[:, inner_width:]).astype(
            jnp.bfloat16
        )
        product = jnp.dot(hidden, down_weight[local], preferred_element_type=jnp.float32)
        total = total + share[:, None] * product
    return lax.psum_scatter(total.astype(jnp.bfloat16), AXES, scatter_dimension=0, tiled=True)


RATE = dict(z=1.405, y=1.405, lat=2.1, up=0.75, dn=0.5, hid=0.4, sum=0.12, op=0.04, w0=11.0, w1=17.0, depth=2.5, meta=0.2)

def rank(style, b, top):
    if style == 'near': return b
    if style == 'far': return top - b
    return 0 if b == 0 else top + 1 - b

def plan(line, pieces, ag, rs, style='nf', cstyle='nf', rate=None, sidefirst=True, own=1.5, tweak=None):
    R = dict(RATE); R.update(rate or {})
    L, P = line, pieces
    META = P
    time_of, waiting, avail, link, clock = {}, {}, [[] for _ in range(L)], {}, [0.0]*L
    order = [[] for _ in range(L)]
    count = 0
    def post(event, t):
        time_of[event] = t
        for op in waiting.pop(event, ()):
            op['need'] -= 1
            op['ready'] = max(op['ready'], t)
            if op['need'] == 0: avail[op['z']].append(op)
    ops = []
    def add(z, name, deps, key, lk=None):
        op = dict(z=z, name=name, need=0, ready=0.0, key=key, link=lk)
        for d in set(deps):
            waiting.setdefault(d, []).append(op); op['need'] += 1
        ops.append(op)
        if op['need'] == 0: avail[z].append(op)
        return op
    sf = (lambda p: -p) if sidefirst else (lambda p: p)
    for z in range(L):
        for j in range(L):
            d = abs(j - z)
            dist = own if d == 0 else d
            crank = rank(cstyle, d-1, L-2) if d else own
            for lk, step, ends in (('u', 1, L-1), ('d', -1, 0)):
                if z == ends or (j - z)*step > 0: continue
                top = z if step > 0 else L-1-z
                a = rank(style, d, top)
                for p in list(range(P)) + [META]:
                    for r in ((0,) if p < ag[j] or p == META else (0, 1)):
                        add(z, ('AGZ', j, r, p, lk), [('t', z, j, r, p)], (0, a, p != META, sf(p), r), lk)
            for p in list(range(P)) + [META]:
                if p < ag[j] or p == META or j == z:
                    add(z, ('AGY', j, 0, p), [('t', z, j, 0, p)], (0, crank if j != z else -1, p != META, sf(p)), 'y')
            for p in range(P):
                add(z, ('UP', j, p), [('t', z, j, 0, p), ('t', z, j, 1, p), ('w0', z)], (3, crank, sf(p)))
                add(z, ('DN', j, p), [('h', z, j), ('w1', z)], (2, crank, sf(p)))
            add(z, ('HID', j), [('a', z, j, p) for p in range(P)] + [('t', z, j, 0, META), ('t', z, j, 1, META)], (2, crank, -99))
            for p in range(rs[j]):
                add(z, ('NEAR', j, p), [('p', z, j, p)], (1, crank, sf(p)), 'y')
            for p in range(P):
                main = p < rs[j]
                for r in ((0,) if main else (1, 0)):
                    deps = [('p', z, j, p)]
                    if j == z:
                        if z > 0: deps.append(('c', z, z, r, p))
                        if z < L-1: deps.append(('c', z, L, r, p))
                        if r == 0: deps.append(('n', z, z, p))
                        add(z, ('FIN', r, p), deps, (1, -1 if r == 1 else 9, sf(p)), 'y' if r == 1 else None)
                    else:
                        if main: deps.append(('n', z, j, p))
                        came = z > 0 if j > z else z < L-1
                        if came: deps.append(('c', z, j, r, p))
                        add(z, ('SUM', j, r, p), deps, (1, crank, sf(p), -r), 'u' if j > z else 'd')
    for z in range(L):
        for lk in 'udy': link[z, lk] = 0.0
        for p in range(P+1): post(('t', z, z, 0, p), 0.0)
        post(('w0', z), R['w0']); post(('w1', z), R['w1'])
    def send(z, lk, t, size):
        e = max(t, link[z, lk]) + size
        link[z, lk] = e
        return e + R['lat']
    left = len(ops)
    while left:
        best = None
        for z in range(L):
            if not avail[z]: continue
            st = min(max(o['ready'], link[z, o['link']] - R['depth']) if o['link'] else o['ready'] for o in avail[z])
            st = max(st, clock[z])
            if best is None or st < best[0]: best = (st, z)
        t, z = best
        cand = [o for o in avail[z] if o['ready'] <= t + 1e-9 and (not o['link'] or link[z, o['link']] - R['depth'] <= t + 1e-9)]
        op = min(cand, key=lambda o: o['key'])
        avail[z].remove(op)
        left -= 1
        n = op['name']; k = n[0]
        if k in ('AGZ', 'AGY'):
            te = t + R['op']
            size = R['meta'] if n[3] == META else R['y' if k == 'AGY' else 'z']
            if k == 'AGY': te2 = send(z, 'y', te, size); post(('t', z, n[1], 1, n[3]), te2)
            else:
                te2 = send(z, n[4], te, size)
                post(('t', z + (1 if n[4] == 'u' else -1), n[1], n[2], n[3]), te2)
        elif k == 'UP':
            te = t + R['up']; post(('a', z, n[1], n[2]), te)
        elif k == 'HID':
            te = t + R['hid']; post(('h', z, n[1]), te)
        elif k == 'DN':
            te = t + R['dn']; post(('p', z, n[1], n[2]), te)
        elif k == 'NEAR':
            te = t + R['op']; post(('n', z, n[1], n[2]), send(z, 'y', te, R['y']))
        elif k == 'SUM':
            te = t + R['sum']; up = n[1] > z; zz = z + (1 if up else -1)
            slot = L if (zz == n[1] and not up) else n[1]
            post(('c', zz, slot, n[2], n[3]), send(z, 'u' if up else 'd', te, R['z']))
        elif k == 'FIN':
            te = t + R['sum']
            if n[1] == 1: post(('n', z, z, n[2]), send(z, 'y', te, R['y']))
        clock[z] = te
        order[z].append((t, te, n))
    return order, max(clock), link


def pieces_of(width):
    return max(n for n in range(1, 8) if width % (n * LANES) == 0)


def splits(line, pieces):
    ends = round(pieces * 5 / 7)
    return (ends,) * line, (ends,) * line


PAIR = 2
LANES = 128
VMEM_BYTES = 60 * 1024 * 1024
MESH = pl.DeviceIdType.MESH
HEAVY = {"NONE": 0, "UP": 1, "HID": 2, "DN": 3, "SUM": 4}
UP_TO, DOWN_TO, SIDE_TO, HERE = 0, 1, 2, 3


def steps_of(line, pieces, ag, rs, order):
    programs = []
    for z in range(line):
        steps, seen, drains = [], set(), []

        def emit(op, j=0, r=0, p=0, dest=0, slot=0, near=0, below=0, above=0):
            steps.append((op, j, r, p, dest, slot, near, below, above))

        def drain(t, *step):
            drains.append((t, step))

        def need(j, r, p):
            if (j, r, p) in seen:
                return
            seen.add((j, r, p))
            if j == z and r == 0:
                if "own" not in seen:
                    seen.add("own")
                    emit("OWN")
            elif p == pieces:
                emit("RTM", j, r)
            else:
                emit("RT", j, r, p)

        def weight(which):
            if which not in seen:
                seen.add(which)
                emit(which)

        for start, end, n in order[z]:
            while drains and drains[0][0] < start - DRAIN_AFTER:
                emit(*drains.pop(0)[1])
            k = n[0]
            if k == "AGZ":
                _, j, r, p, lk = n
                need(j, r, p)
                dest = UP_TO if lk == "u" else DOWN_TO
                slot = line if j == z and dest == DOWN_TO else j
                if p == pieces:
                    emit("AGZM", j, r, 0, dest, slot)
                    drain(start, "DZM", j, r, 0, dest, slot)
                else:
                    emit("AGZ", j, r, p, dest, slot)
                    drain(start, "DZ", j, r, p, dest, slot)
            elif k == "AGY":
                _, j, r, p = n
                need(j, r, p)
                if p == pieces:
                    emit("AGYM", j)
                    drain(start, "DYM", j)
                else:
                    emit("AGY", j, 0, p)
                    drain(start, "DY", j, 0, p)
            elif k == "UP":
                need(n[1], 0, n[2])
                need(n[1], 1, n[2])
                weight("W0")
                emit("UP", n[1], 0, n[2])
            elif k == "HID":
                need(n[1], 0, pieces)
                need(n[1], 1, pieces)
                emit("HID", n[1])
            elif k == "DN":
                weight("W1")
                emit("DN", n[1], 0, n[2])
            elif k == "NEAR":
                emit("NEAR", n[1], 0, n[2])
                drain(start, "DN_S", n[1], 0, n[2])
            elif k == "SUM":
                _, j, r, p = n
                up = j > z
                far = j == z - 1
                came = z > 0 if up else z < line - 1
                dest = UP_TO if up else DOWN_TO
                slot = line if far else j
                emit("SUM", j, r, p, dest, slot, int(p < rs[j]), int(came))
                drain(start, "DC", j, r, p, dest, slot)
            elif k == "FIN":
                _, r, p = n
                dest = SIDE_TO if r == 1 else HERE
                emit("SUM", z, r, p, dest, z, int(r == 0), int(z > 0), int(z < line - 1))
                if r == 1:
                    drain(start, "DN_S", z, 0, p)
        for _, step in drains:
            emit(*step)
        programs.append(grouped(steps))
    longest = max(len(p) for p in programs)
    return [p + [([], ("NONE",))] * (longest - len(p)) for p in programs]


def grouped(steps):
    groups, light = [], []
    for fields in steps:
        if fields[0] in HEAVY:
            groups.append((light, fields))
            light = []
        else:
            light.append(fields)
    return groups + [(light, ("NONE",))]


FIELDS = ((8, "op"), (16, "j"), (2, "r"), (32, "p"), (4, "dest"), (16, "slot"), (2, "near"), (2, "below"), (2, "above"))


def packed(step):
    word, scale = 0, 1
    for (size, _), value in zip(FIELDS, (HEAVY[step[0]],) + tuple(step[1:])):
        word += value * scale
        scale *= size
    return word


def kernel(
    line, pieces, experts, programs, ids_ref, gate_ref, x_hbm, wgu_hbm, wd_hbm, out_ref,
    tok, meta, part, near, chain, wg, wd, acc, hid, share, tot,
    x_sem, w_l, w_s, w_r, tok_r, zs, ys, near_r, near_s, chain_r, chain_s,
):
    rows, width = out_ref.shape
    inner = wd.shape[1]
    block = width // pieces
    e = lax.axis_index("ep")
    c = lax.axis_index("node")
    z, y = e // PAIR, e % PAIR
    other = 1 - y
    has_dn, has_up = z > 0, z < line - 1
    to_up, to_dn = {"ep": e + PAIR}, {"ep": e - PAIR}
    to_y, to_core = {"ep": z * PAIR + other}, {"node": 1 - c}

    own_copy = pltpu.make_async_copy(x_hbm, tok.at[z, y], x_sem)
    own_copy.start()
    local = [
        pltpu.make_async_copy(wgu_hbm.at[0], wg.at[0], w_l.at[0]),
        pltpu.make_async_copy(wd_hbm.at[0], wd.at[0], w_l.at[1]),
    ]
    for copy in local:
        copy.start()

    barrier = pltpu.get_barrier_semaphore()

    def greet(target):
        pl.semaphore_signal(barrier, inc=1, device_id=target, device_id_type=MESH)

    greet(to_core)
    greet(to_y)
    pl.when(has_up)(lambda: greet(to_up))
    pl.when(has_dn)(lambda: greet(to_dn))

    lane = lax.broadcasted_iota(jnp.int32, (rows, LANES), 1)
    name = jnp.where(lane < experts, lane, lane - experts)
    total = jnp.zeros((rows, LANES), jnp.float32)
    for k in range(ids_ref.shape[1]):
        total += jnp.where(ids_ref[:, k : k + 1] == name, gate_ref[:, k : k + 1], 0.0)
    high = total.astype(jnp.bfloat16)
    low = (total - high.astype(jnp.float32)).astype(jnp.bfloat16)
    wide = jnp.where(lane < experts, high.astype(jnp.float32), low.astype(jnp.float32))
    meta[z, y] = jnp.where(lane < 2 * experts, wide, 0.0).astype(jnp.bfloat16)
    acc[...] = jnp.zeros_like(acc)

    pl.semaphore_wait(barrier, 2 + jnp.where(has_up, 1, 0) + jnp.where(has_dn, 1, 0))

    def remote(src, dst, s, r, target):
        return pltpu.make_async_remote_copy(
            src_ref=src, dst_ref=dst, send_sem=s, recv_sem=r,
            device_id=target, device_id_type=MESH,
        )

    swapped = [
        remote(wgu_hbm.at[0], wg.at[1], w_s.at[0], w_r.at[0], to_core),
        remote(wd_hbm.at[0], wd.at[1], w_s.at[1], w_r.at[1], to_core),
    ]
    for copy in swapped:
        copy.start()
    mine = e * 2 + c
    names = (mine, e * 2 + 1 - c)

    def span(p):
        return pl.ds(pl.multiple_of(p * block, LANES), block)

    def tok_copy(j, row, p, s, target):
        ref = tok.at[j, row, :, span(p)]
        return remote(ref, ref, s, tok_r.at[j, row, p], target)

    def meta_copy(j, row, s, target):
        ref = meta.at[j, row]
        return remote(ref, ref, s, tok_r.at[j, row, pieces], target)

    def both_ways(dest, act):
        pl.when(dest == UP_TO)(lambda: act(to_up))
        pl.when(dest == DOWN_TO)(lambda: act(to_dn))

    def near_copy(j, src, p):
        return remote(
            src.at[:, span(p)], near.at[j, :, span(p)], near_s.at[j, p], near_r.at[j, p], to_y
        )

    def chain_copy(j, row, p, slot, target):
        return remote(
            part.at[j, row, :, span(p)], chain.at[slot, row, :, span(p)],
            chain_s.at[j, row, p], chain_r.at[slot, row, p], target,
        )

    def up(j, p):
        at = span(p)
        rows_in = tok[j, :, :, at].reshape(PAIR * rows, block)
        for s in range(2):
            acc[j, s] += jnp.dot(rows_in, wg[s, at, :], preferred_element_type=jnp.float32)

    def hidden(j):
        for s in range(2):
            gate, over = acc[j, s, :, :inner], acc[j, s, :, inner:]
            hid[j, s] = (jax.nn.silu(gate) * over).astype(jnp.bfloat16)
        parts = meta[j].astype(jnp.float32).reshape(PAIR * rows, LANES)
        at = lax.broadcasted_iota(jnp.int32, parts.shape, 1)
        for s, expert in enumerate(names):
            kept = jnp.where((at == expert) | (at == expert + experts), parts, 0.0)
            share[j, s] = jnp.broadcast_to(
                jnp.sum(kept, axis=1, keepdims=True), (PAIR * rows, LANES)
            )

    def down(j, p):
        at = span(p)
        total = 0.0
        for s in range(2):
            product = jnp.dot(hid[j, s], wd[s, :, at], preferred_element_type=jnp.float32)
            total += share[j, s, :, :1] * product
        part[j, :, :, at] = total.astype(jnp.bfloat16).reshape(PAIR, rows, block)

    def sums(j, row, p, dest, slot, f_near, f_below, f_above):
        at = span(p)
        tot[...] = part[j, row, :, at].astype(jnp.float32)

        @pl.when(f_near == 1)
        def _():
            near_copy(j, part.at[j, row], p).wait_recv()
            tot[...] += near[j, :, at].astype(jnp.float32)

        @pl.when(f_below == 1)
        def _():
            chain_copy(j, row, p, j, to_y).wait_recv()
            tot[...] += chain[j, row, :, at].astype(jnp.float32)

        @pl.when(f_above == 1)
        def _():
            chain_copy(j, row, p, line, to_y).wait_recv()
            tot[...] += chain[line, row, :, at].astype(jnp.float32)

        value = tot[...].astype(jnp.bfloat16)

        @pl.when(dest == HERE)
        def _():
            out_ref[:, at] = value

        @pl.when(dest != HERE)
        def _():
            part[j, row, :, at] = value
            both_ways(dest, lambda target: chain_copy(j, row, p, slot, target).start())
            pl.when(dest == SIDE_TO)(lambda: near_copy(j, part.at[j, row], p).start())

    def light(fields):
        name, j, r, p, dest, slot = fields[:6]
        row = other if r else y
        target = to_up if dest == UP_TO else to_dn
        if name == "RT":
            tok_copy(j, row, p, x_sem, to_y).wait_recv()
        elif name == "RTM":
            meta_copy(j, row, x_sem, to_y).wait_recv()
        elif name == "AGZ":
            tok_copy(j, row, p, zs.at[slot, r, p], target).start()
        elif name == "AGZM":
            meta_copy(j, row, zs.at[slot, r, pieces], target).start()
        elif name == "AGY":
            tok_copy(j, y, p, ys.at[j, p], to_y).start()
        elif name == "AGYM":
            meta_copy(j, y, ys.at[j, pieces], to_y).start()
        elif name == "NEAR":
            near_copy(j, part.at[j, other], p).start()
        elif name == "W0":
            local[0].wait()
            swapped[0].wait_recv()
        elif name == "W1":
            local[1].wait()
            swapped[1].wait_recv()
        elif name == "DZ":
            tok_copy(j, row, p, zs.at[slot, r, p], to_y).wait_send()
        elif name == "DZM":
            meta_copy(j, row, zs.at[slot, r, pieces], to_y).wait_send()
        elif name == "DY":
            tok_copy(j, y, p, ys.at[j, p], to_y).wait_send()
        elif name == "DYM":
            meta_copy(j, y, ys.at[j, pieces], to_y).wait_send()
        elif name == "DN_S":
            near_copy(j, part.at[j, other], p).wait_send()
        elif name == "DC":
            chain_copy(j, row, p, slot, to_y).wait_send()
        elif name == "OWN":
            own_copy.wait()

    def branch(m, program, low, high):
        if high - low == 1:
            for fields in program[low][0]:
                light(fields)
            return jnp.int32(packed(program[low][1]))
        half = (low + high) // 2
        return lax.cond(
            m < half, lambda: branch(m, program, low, half), lambda: branch(m, program, half, high)
        )

    def place(m, low, high):
        if high - low == 1:
            return branch(m, programs[low], 0, len(programs[low]))
        half = (low + high) // 2
        return lax.cond(z < half, lambda: place(m, low, half), lambda: place(m, half, high))

    def step(m, carry):
        word = place(m, 0, line)
        fields = []
        for size, _ in FIELDS:
            fields.append(lax.rem(word, jnp.int32(size)))
            word = lax.div(word, jnp.int32(size))
        op, j, r, p, dest, slot, f_near, f_below, f_above = fields
        row = jnp.where(r == 0, y, other)
        pl.when(op == HEAVY["UP"])(lambda: up(j, p))
        pl.when(op == HEAVY["HID"])(lambda: hidden(j))
        pl.when(op == HEAVY["DN"])(lambda: down(j, p))
        pl.when(op == HEAVY["SUM"])(lambda: sums(j, row, p, dest, slot, f_near, f_below, f_above))
        return carry

    lax.fori_loop(0, len(programs[0]), step, 0)
    for copy in swapped:
        copy.wait_send()


def on_grid(line, tokens, expert_ids, gate_weights, gate_up_weight, down_weight):
    experts = lax.axis_size("ep") * lax.axis_size("node")
    rows, width = tokens.shape
    inner = down_weight.shape[1]
    pieces = pieces_of(width)
    ag, rs = splits(line, pieces)
    order = plan(line, pieces, ag, rs)[0]
    programs = steps_of(line, pieces, ag, rs, order)
    dma, vmem, bf = pltpu.SemaphoreType.DMA, pltpu.VMEM, jnp.bfloat16
    return pl.pallas_call(
        functools.partial(kernel, line, pieces, experts, programs),
        out_shape=jax.ShapeDtypeStruct((rows, width), bf),
        in_specs=[
            pl.BlockSpec(memory_space=pltpu.VMEM),
            pl.BlockSpec(memory_space=pltpu.VMEM),
            pl.BlockSpec(memory_space=pl.ANY),
            pl.BlockSpec(memory_space=pl.ANY),
            pl.BlockSpec(memory_space=pl.ANY),
        ],
        out_specs=pl.BlockSpec(memory_space=pltpu.VMEM),
        scratch_shapes=[
            vmem((line, PAIR, rows, width), bf),
            vmem((line, PAIR, rows, LANES), bf),
            vmem((line, PAIR, rows, width), bf),
            vmem((line, rows, width), bf),
            vmem((line + 1, PAIR, rows, width), bf),
            vmem((2, width, 2 * inner), bf),
            vmem((2, inner, width), bf),
            vmem((line, 2, PAIR * rows, 2 * inner), jnp.float32),
            vmem((line, 2, PAIR * rows, inner), bf),
            vmem((line, 2, PAIR * rows, LANES), jnp.float32),
            vmem((rows, width // pieces), jnp.float32),
            dma(()), dma((2,)), dma((2,)), dma((2,)),
            dma((line, PAIR, pieces + 1)), dma((line + 1, PAIR, pieces + 1)),
            dma((line, pieces + 1)), dma((line, pieces)), dma((line, pieces)),
            dma((line + 1, PAIR, pieces)), dma((line, PAIR, pieces)),
        ],
        compiler_params=pltpu.CompilerParams(
            collective_id=0, has_side_effects=True, vmem_limit_bytes=VMEM_BYTES
        ),
    )(expert_ids, gate_weights, tokens, gate_up_weight, down_weight)


def on_device(tokens, expert_ids, gate_weights, gate_up_weight, down_weight):
    chips, cores = lax.axis_size("ep"), lax.axis_size("node")
    line = chips // PAIR
    rows, width = tokens.shape
    inner = down_weight.shape[1]
    planes = (6 * line + 3 * PAIR) * rows * width * 2 + 6 * inner * width * 2 * 1.1
    args = (tokens, expert_ids, gate_weights, gate_up_weight, down_weight)
    fits = planes < 0.9 * VMEM_BYTES and gate_up_weight.shape[0] == 1
    fits = fits and 2 * chips * cores <= LANES and pieces_of(width) > 1
    paired = cores == 2 and lax.axis_size("groups") * PAIR == 4
    if fits and paired and chips % PAIR == 0 and 1 < line < 9:
        return on_grid(line, *args)
    return spread_out(*args)


def solution(mesh):
    placed = (
        P(("groups", "ep", "node"), None),
        P(("groups", "ep", "node"), None),
        P(("groups", "ep", "node"), None),
        P(("ep", "node"), None, None),
        P(("ep", "node"), None, None),
    )
    return jax.shard_map(
        on_device,
        mesh=mesh,
        in_specs=placed,
        out_specs=P(("groups", "ep", "node"), None),
        check_vma=False,
    )
```

```python
import functools

import jax
import jax.numpy as jnp
from jax import lax
from jax.experimental import pallas as pl
from jax.experimental.pallas import tpu as pltpu
from jax.sharding import PartitionSpec as P

AXES = ("ep", "node")
DRAIN_AFTER = 8.0


def spread_out(tokens, expert_ids, gate_weights, gate_up_weight, down_weight):
    local_count, inner_width = down_weight.shape[0], down_weight.shape[1]
    device = lax.axis_index("ep") * lax.axis_size("node") + lax.axis_index("node")
    all_tokens = lax.all_gather(tokens, AXES, axis=0, tiled=True)
    all_ids = lax.all_gather(expert_ids, AXES, axis=0, tiled=True)
    all_weights = lax.all_gather(gate_weights, AXES, axis=0, tiled=True)
    total = 0.0
    for local in range(local_count):
        expert = device * local_count + local
        share = jnp.sum(jnp.where(all_ids == expert, all_weights, 0.0), axis=1)
        gate_up = jnp.dot(all_tokens, gate_up_weight[local], preferred_element_type=jnp.float32)
        hidden = (jax.nn.silu(gate_up[:, :inner_width]) * gate_up[:, inner_width:]).astype(
            jnp.bfloat16
        )
        product = jnp.dot(hidden, down_weight[local], preferred_element_type=jnp.float32)
        total = total + share[:, None] * product
    return lax.psum_scatter(total.astype(jnp.bfloat16), AXES, scatter_dimension=0, tiled=True)


RATE = dict(z=1.46, y=1.46, lat=2.1, up=0.46, dn=0.42, hid=0.85, sum=0.2, op=0.06, w0=13.0, w1=19.0, depth=2.5, meta=0.2)

def rank(style, b, top):
    if style == 'near': return b
    if style == 'far': return top - b
    return 0 if b == 0 else top + 1 - b

def plan(line, pieces, ag, rs, style='nf', cstyle='nf', rate=None, sidefirst=True, own=1.5, tweak=None):
    R = dict(RATE); R.update(rate or {})
    L, P = line, pieces
    META = P
    time_of, waiting, avail, link, clock = {}, {}, [[] for _ in range(L)], {}, [0.0]*L
    order = [[] for _ in range(L)]
    count = 0
    def post(event, t):
        time_of[event] = t
        for op in waiting.pop(event, ()):
            op['need'] -= 1
            op['ready'] = max(op['ready'], t)
            if op['need'] == 0: avail[op['z']].append(op)
    ops = []
    def add(z, name, deps, key, lk=None):
        g = (z, name[0], name[1] if name[0] != 'FIN' else z, name[2] >= META if name[0] == 'AGY' else (name[4] if name[0] == 'AGZ' else 0))
        if tweak: key = (key[0] * 100 + key[1] * 10 + tweak.get(g, 0),) + key[2:]
        op = dict(z=z, name=name, need=0, ready=0.0, key=key, link=lk)
        for d in set(deps):
            waiting.setdefault(d, []).append(op); op['need'] += 1
        ops.append(op)
        if op['need'] == 0: avail[z].append(op)
        return op
    sf = (lambda p: -p) if sidefirst else (lambda p: p)
    for z in range(L):
        for j in range(L):
            d = abs(j - z)
            dist = own if d == 0 else d
            crank = rank(cstyle, d-1, L-2) if d else own
            for lk, step, ends in (('u', 1, L-1), ('d', -1, 0)):
                if z == ends or (j - z)*step > 0: continue
                top = z if step > 0 else L-1-z
                a = rank(style, d, top)
                for p in list(range(P)) + [META]:
                    for r in ((0,) if p < ag[j] else (0, 1)):
                        add(z, ('AGZ', j, r, p, lk), [('t', z, j, r, p)], (0, a, p != META, sf(p), r), lk)
            for p in list(range(P)) + [META]:
                if p < ag[j] or j == z:
                    add(z, ('AGY', j, 0, p), [('t', z, j, 0, p)], (0, crank if j != z else -1, p != META, sf(p)), 'y')
            for p in range(P):
                add(z, ('UP', j, p), [('t', z, j, 0, p), ('t', z, j, 1, p), ('w0', z)], (3, crank, sf(p)))
                add(z, ('DN', j, p), [('h', z, j), ('w1', z)], (2, crank, sf(p)))
            add(z, ('HID', j), [('a', z, j, p) for p in range(P)] + [('t', z, j, 0, META), ('t', z, j, 1, META)], (2, crank, -99))
            for p in range(rs[j]):
                add(z, ('NEAR', j, p), [('p', z, j, p)], (1, crank, sf(p)), 'y')
            for p in range(P):
                main = p < rs[j]
                for r in ((0,) if main else (1, 0)):
                    deps = [('p', z, j, p)]
                    if j == z:
                        if z > 0: deps.append(('c', z, z, r, p))
                        if z < L-1: deps.append(('c', z, L, r, p))
                        if r == 0: deps.append(('n', z, z, p))
                        add(z, ('FIN', r, p), deps, (1, -1 if r == 1 else 9, sf(p)), 'y' if r == 1 else None)
                    else:
                        if main: deps.append(('n', z, j, p))
                        came = z > 0 if j > z else z < L-1
                        if came: deps.append(('c', z, j, r, p))
                        add(z, ('SUM', j, r, p), deps, (1, crank, sf(p), -r), 'u' if j > z else 'd')
    for z in range(L):
        for lk in 'udy': link[z, lk] = 0.0
        for p in range(P+1): post(('t', z, z, 0, p), 0.0)
        post(('w0', z), R['w0']); post(('w1', z), R['w1'])
    def send(z, lk, t, size):
        e = max(t, link[z, lk]) + size
        link[z, lk] = e
        return e + R['lat']
    left = len(ops)
    while left:
        best = None
        for z in range(L):
            if not avail[z]: continue
            st = min(max(o['ready'], link[z, o['link']] - R['depth']) if o['link'] else o['ready'] for o in avail[z])
            st = max(st, clock[z])
            if best is None or st < best[0]: best = (st, z)
        t, z = best
        cand = [o for o in avail[z] if o['ready'] <= t + 1e-9 and (not o['link'] or link[z, o['link']] - R['depth'] <= t + 1e-9)]
        op = min(cand, key=lambda o: o['key'])
        avail[z].remove(op)
        left -= 1
        n = op['name']; k = n[0]
        if k in ('AGZ', 'AGY'):
            te = t + R['op']
            size = R['meta'] if n[3] == META else R['y' if k == 'AGY' else 'z']
            if k == 'AGY': te2 = send(z, 'y', te, size); post(('t', z, n[1], 1, n[3]), te2)
            else:
                te2 = send(z, n[4], te, size)
                post(('t', z + (1 if n[4] == 'u' else -1), n[1], n[2], n[3]), te2)
        elif k == 'UP':
            te = t + R['up']; post(('a', z, n[1], n[2]), te)
        elif k == 'HID':
            te = t + R['hid']; post(('h', z, n[1]), te)
        elif k == 'DN':
            te = t + R['dn']; post(('p', z, n[1], n[2]), te)
        elif k == 'NEAR':
            te = t + R['op']; post(('n', z, n[1], n[2]), send(z, 'y', te, R['y']))
        elif k == 'SUM':
            te = t + R['sum']; up = n[1] > z; zz = z + (1 if up else -1)
            slot = L if (zz == n[1] and not up) else n[1]
            post(('c', zz, slot, n[2], n[3]), send(z, 'u' if up else 'd', te, R['z']))
        elif k == 'FIN':
            te = t + R['sum']
            if n[1] == 1: post(('n', z, z, n[2]), send(z, 'y', te, R['y']))
        clock[z] = te
        order[z].append((t, te, n))
    return order, max(clock), link


RATES7 = dict(z=1.405, y=1.405)
MOST = 7
AG, RS = (0.42857142857142855, 0.7142857142857143, 0.7142857142857143, 0.42857142857142855), (0.7142857142857143, 0.8571428571428571, 0.8571428571428571, 0.7142857142857143)
SHIFTS = {
    (0, 'AGY', 0, False): -13.36, (0, 'AGY', 0, True): -13.36, (0, 'AGY', 1, False): 55.81, (0, 'AGY', 1, True): 55.81,
    (0, 'AGY', 2, False): -41.77, (0, 'AGY', 2, True): -41.77, (0, 'AGY', 3, False): 45.21, (0, 'AGY', 3, True): 45.21,
    (0, 'AGZ', 0, 'd'): 249.9, (0, 'AGZ', 0, 'u'): 149.1, (0, 'AGZ', 1, 'd'): -51.32, (0, 'AGZ', 1, 'u'): 248.12,
    (0, 'AGZ', 2, 'd'): -205.81, (0, 'AGZ', 2, 'u'): -388.16, (0, 'AGZ', 3, 'd'): 28.9, (0, 'AGZ', 3, 'u'): -24.01,
    (0, 'DN', 0, 0): 177.24, (0, 'DN', 1, 0): 60.14, (0, 'DN', 2, 0): -31.2, (0, 'DN', 3, 0): -54.23,
    (0, 'FIN', 0, 0): -228.62, (0, 'FIN', 1, 0): -133.78, (0, 'FIN', 2, 0): -56.6, (0, 'FIN', 3, 0): -190.02,
    (0, 'HID', 0, 0): 158.13, (0, 'HID', 1, 0): -225.39, (0, 'HID', 2, 0): -117.65, (0, 'HID', 3, 0): -188.31,
    (0, 'NEAR', 0, 0): 197.15, (0, 'NEAR', 1, 0): -14.44, (0, 'NEAR', 2, 0): 25.08, (0, 'NEAR', 3, 0): 57.56,
    (0, 'SUM', 0, 0): -178.14, (0, 'SUM', 1, 0): 57.5, (0, 'SUM', 2, 0): -11.22, (0, 'SUM', 3, 0): -195.43,
    (0, 'UP', 0, 0): -43.36, (0, 'UP', 1, 0): 93.3, (0, 'UP', 2, 0): 91.86, (0, 'UP', 3, 0): 388.72,
    (1, 'AGY', 0, False): 7.02, (1, 'AGY', 0, True): 7.02, (1, 'AGY', 1, False): -73.06, (1, 'AGY', 1, True): -73.06,
    (1, 'AGY', 2, False): -103.05, (1, 'AGY', 2, True): -103.05, (1, 'AGY', 3, False): -13.81, (1, 'AGY', 3, True): -13.81,
    (1, 'AGZ', 0, 'd'): 59.55, (1, 'AGZ', 0, 'u'): 214.1, (1, 'AGZ', 1, 'd'): 139.45, (1, 'AGZ', 1, 'u'): -89.69,
    (1, 'AGZ', 2, 'd'): 54.75, (1, 'AGZ', 2, 'u'): 14.06, (1, 'AGZ', 3, 'd'): 33.13, (1, 'AGZ', 3, 'u'): 190.08,
    (1, 'DN', 0, 0): 207.18, (1, 'DN', 1, 0): 380.58, (1, 'DN', 2, 0): 228.14, (1, 'DN', 3, 0): -9.15,
    (1, 'FIN', 0, 0): -45.27, (1, 'FIN', 1, 0): -130.65, (1, 'FIN', 2, 0): 97.6, (1, 'FIN', 3, 0): 118.78,
    (1, 'HID', 0, 0): 337.71, (1, 'HID', 1, 0): -167.34, (1, 'HID', 2, 0): 364.56, (1, 'HID', 3, 0): 212.02,
    (1, 'NEAR', 0, 0): -91.18, (1, 'NEAR', 1, 0): 89.49, (1, 'NEAR', 2, 0): -51.23, (1, 'NEAR', 3, 0): -61.51,
    (1, 'SUM', 0, 0): 150.15, (1, 'SUM', 1, 0): 119.84, (1, 'SUM', 2, 0): -42.83, (1, 'SUM', 3, 0): -64.48,
    (1, 'UP', 0, 0): -117.22, (1, 'UP', 1, 0): -93.07, (1, 'UP', 2, 0): -90.3, (1, 'UP', 3, 0): -53.25,
}
STYLE = dict(style='far', cstyle='far', rate={'z': 1.46, 'y': 1.46, 'up': 0.45999999999999996, 'dn': 0.42000000000000004, 'sum': 0.2, 'depth': 0.8}, sidefirst=False, own=1.5, tweak=None)


def mirrored(line, shifts):
    turned = {"u": "d", "d": "u"}
    both = dict(shifts)
    for (z, name, j, way), value in shifts.items():
        both[line - 1 - z, name, line - 1 - j, turned.get(way, way)] = value
    return both


def pieces_of(width):
    return max(n for n in range(1, MOST + 1) if width % (n * LANES) == 0)


def splits(line, pieces):
    pick = lambda part: tuple(round(pieces * part[min(j, line - 1 - j)]) for j in range(line))
    return pick(AG), pick(RS)


PAIR = 2
LANES = 128
VMEM_BYTES = 55_900_000
MESH = pl.DeviceIdType.MESH
HEAVY = {"NONE": 0, "UP": 1, "HID": 2, "DN": 3, "SUM": 4}
UP_TO, DOWN_TO, SIDE_TO, HERE = 0, 1, 2, 3


def steps_of(line, pieces, ag, rs, order):
    programs = []
    for z in range(line):
        steps, seen, drains = [], set(), []

        def emit(op, j=0, r=0, p=0, dest=0, slot=0, near=0, below=0, above=0):
            steps.append((op, j, r, p, dest, slot, near, below, above))

        def drain(t, *step):
            drains.append((t, step))

        def need(j, r, p):
            if (j, r, p) in seen:
                return
            seen.add((j, r, p))
            if j == z and r == 0:
                if "own" not in seen:
                    seen.add("own")
                    emit("OWN")
            elif p == pieces:
                emit("RTM", j, r)
            else:
                emit("RT", j, r, p)

        def weight(which):
            if which not in seen:
                seen.add(which)
                emit(which)

        for start, end, n in order[z]:
            while drains and drains[0][0] < start - DRAIN_AFTER:
                emit(*drains.pop(0)[1])
            k = n[0]
            if k == "AGZ":
                _, j, r, p, lk = n
                need(j, r, p)
                dest = UP_TO if lk == "u" else DOWN_TO
                slot = line if j == z and dest == DOWN_TO else j
                if p == pieces:
                    emit("AGZM", j, r, 0, dest, slot)
                    drain(start, "DZM", j, r, 0, dest, slot)
                else:
                    emit("AGZ", j, r, p, dest, slot)
                    drain(start, "DZ", j, r, p, dest, slot)
            elif k == "AGY":
                _, j, r, p = n
                need(j, r, p)
                if p == pieces:
                    emit("AGYM", j)
                    drain(start, "DYM", j)
                else:
                    emit("AGY", j, 0, p)
                    drain(start, "DY", j, 0, p)
            elif k == "UP":
                need(n[1], 0, n[2])
                need(n[1], 1, n[2])
                weight("W0")
                emit("UP", n[1], 0, n[2])
            elif k == "HID":
                need(n[1], 0, pieces)
                need(n[1], 1, pieces)
                emit("HID", n[1])
            elif k == "DN":
                weight("W1")
                emit("DN", n[1], 0, n[2])
            elif k == "NEAR":
                emit("NEAR", n[1], 0, n[2])
                drain(start, "DN_S", n[1], 0, n[2])
            elif k == "SUM":
                _, j, r, p = n
                up = j > z
                far = j == z - 1
                came = z > 0 if up else z < line - 1
                dest = UP_TO if up else DOWN_TO
                slot = line if far else j
                emit("SUM", j, r, p, dest, slot, int(p < rs[j]), int(came))
                drain(start, "DC", j, r, p, dest, slot)
            elif k == "FIN":
                _, r, p = n
                dest = SIDE_TO if r == 1 else HERE
                emit("SUM", z, r, p, dest, z, int(r == 0), int(z > 0), int(z < line - 1))
                if r == 1:
                    drain(start, "DN_S", z, 0, p)
        for _, step in drains:
            emit(*step)
        programs.append(grouped(steps))
    longest = max(len(p) for p in programs)
    return [p + [([], ("NONE",))] * (longest - len(p)) for p in programs]


def grouped(steps):
    groups, light = [], []
    for fields in steps:
        if fields[0] in HEAVY:
            groups.append((light, fields))
            light = []
        else:
            light.append(fields)
    return groups + [(light, ("NONE",))]


FIELDS = ((8, "op"), (16, "j"), (2, "r"), (32, "p"), (4, "dest"), (16, "slot"), (2, "near"), (2, "below"), (2, "above"))


def packed(step):
    word, scale = 0, 1
    for (size, _), value in zip(FIELDS, (HEAVY[step[0]],) + tuple(step[1:])):
        word += value * scale
        scale *= size
    return word


def kernel(
    line, pieces, experts, programs, ids_ref, gate_ref, x_hbm, wgu_hbm, wd_hbm, out_ref,
    tok, meta, part, near, chain, wg, wd, acc, hid, share, tot,
    x_sem, w_l, w_s, w_r, tok_r, zs, ys, near_r, near_s, chain_r, chain_s,
):
    rows, width = out_ref.shape
    inner = wd.shape[1]
    block = width // pieces
    e = lax.axis_index("ep")
    c = lax.axis_index("node")
    z, y = e // PAIR, e % PAIR
    other = 1 - y
    has_dn, has_up = z > 0, z < line - 1
    to_up, to_dn = {"ep": e + PAIR}, {"ep": e - PAIR}
    to_y, to_core = {"ep": z * PAIR + other}, {"node": 1 - c}

    own_copy = pltpu.make_async_copy(x_hbm, tok.at[z, y], x_sem)
    own_copy.start()
    local = [
        pltpu.make_async_copy(wgu_hbm.at[0], wg.at[0], w_l.at[0]),
        pltpu.make_async_copy(wd_hbm.at[0], wd.at[0], w_l.at[1]),
    ]
    for copy in local:
        copy.start()

    barrier = pltpu.get_barrier_semaphore()

    def greet(target):
        pl.semaphore_signal(barrier, inc=1, device_id=target, device_id_type=MESH)

    greet(to_core)
    greet(to_y)
    pl.when(has_up)(lambda: greet(to_up))
    pl.when(has_dn)(lambda: greet(to_dn))

    at_row = lax.broadcasted_iota(jnp.int32, (LANES, rows), 0)
    name = jnp.where(at_row < experts, at_row, at_row - experts)
    total = jnp.zeros((LANES, rows), jnp.float32)
    for k in range(ids_ref.shape[0]):
        total += jnp.where(ids_ref[k : k + 1, :] == name, gate_ref[k : k + 1, :], 0.0)
    high = total.astype(jnp.bfloat16).astype(jnp.float32)
    wide = jnp.where(at_row < experts, high, total - high)
    meta[z, y] = jnp.where(at_row < 2 * experts, wide, 0.0).T.astype(jnp.bfloat16)
    acc[...] = jnp.zeros_like(acc)

    pl.semaphore_wait(barrier, 2 + jnp.where(has_up, 1, 0) + jnp.where(has_dn, 1, 0))

    def remote(src, dst, s, r, target):
        return pltpu.make_async_remote_copy(
            src_ref=src, dst_ref=dst, send_sem=s, recv_sem=r,
            device_id=target, device_id_type=MESH,
        )

    swapped = [
        remote(wgu_hbm.at[0], wg.at[1], w_s.at[0], w_r.at[0], to_core),
        remote(wd_hbm.at[0], wd.at[1], w_s.at[1], w_r.at[1], to_core),
    ]
    for copy in swapped:
        copy.start()
    mine = e * 2 + c
    names = (mine, e * 2 + 1 - c)

    def span(p):
        return pl.ds(pl.multiple_of(p * block, LANES), block)

    def tok_copy(j, row, p, s, target):
        ref = tok.at[j, row, :, span(p)]
        return remote(ref, ref, s, tok_r.at[j, row, p], target)

    def meta_copy(j, row, s, target):
        ref = meta.at[j, row]
        return remote(ref, ref, s, tok_r.at[j, row, pieces], target)

    def both_ways(dest, act):
        pl.when(dest == UP_TO)(lambda: act(to_up))
        pl.when(dest == DOWN_TO)(lambda: act(to_dn))

    def near_copy(j, src, p):
        return remote(
            src.at[:, span(p)], near.at[j, :, span(p)], near_s.at[j, p], near_r.at[j, p], to_y
        )

    def chain_copy(j, row, p, slot, target):
        return remote(
            part.at[j, row, :, span(p)], chain.at[slot, row, :, span(p)],
            chain_s.at[j, row, p], chain_r.at[slot, row, p], target,
        )

    def up(j, p):
        at = span(p)
        rows_in = tok[j, :, :, at].reshape(PAIR * rows, block)
        for s in range(2):
            acc[j, s] += jnp.dot(rows_in, wg[s, at, :], preferred_element_type=jnp.float32)

    def hidden(j):
        for s in range(2):
            gate, over = acc[j, s, :, :inner], acc[j, s, :, inner:]
            hid[j, s] = (jax.nn.silu(gate) * over).astype(jnp.bfloat16)
        parts = meta[j].astype(jnp.float32).reshape(PAIR * rows, LANES)
        at = lax.broadcasted_iota(jnp.int32, parts.shape, 1)
        for s, expert in enumerate(names):
            kept = jnp.where((at == expert) | (at == expert + experts), parts, 0.0)
            share[j, s] = jnp.broadcast_to(
                jnp.sum(kept, axis=1, keepdims=True), (PAIR * rows, LANES)
            )

    def down(j, p):
        at = span(p)
        total = 0.0
        for s in range(2):
            product = jnp.dot(hid[j, s], wd[s, :, at], preferred_element_type=jnp.float32)
            total += share[j, s, :, :1] * product
        part[j, :, :, at] = total.astype(jnp.bfloat16).reshape(PAIR, rows, block)

    def sums(j, row, p, dest, slot, f_near, f_below, f_above):
        at = span(p)
        tot[...] = part[j, row, :, at].astype(jnp.float32)

        @pl.when(f_near == 1)
        def _():
            near_copy(j, part.at[j, row], p).wait_recv()
            tot[...] += near[j, :, at].astype(jnp.float32)

        @pl.when(f_below == 1)
        def _():
            chain_copy(j, row, p, j, to_y).wait_recv()
            tot[...] += chain[j, row, :, at].astype(jnp.float32)

        @pl.when(f_above == 1)
        def _():
            chain_copy(j, row, p, line, to_y).wait_recv()
            tot[...] += chain[line, row, :, at].astype(jnp.float32)

        value = tot[...].astype(jnp.bfloat16)

        @pl.when(dest == HERE)
        def _():
            out_ref[:, at] = value

        @pl.when(dest != HERE)
        def _():
            part[j, row, :, at] = value
            both_ways(dest, lambda target: chain_copy(j, row, p, slot, target).start())
            pl.when(dest == SIDE_TO)(lambda: near_copy(j, part.at[j, row], p).start())

    def light(fields):
        name, j, r, p, dest, slot = fields[:6]
        row = other if r else y
        target = to_up if dest == UP_TO else to_dn
        if name == "RT":
            tok_copy(j, row, p, x_sem, to_y).wait_recv()
        elif name == "RTM":
            meta_copy(j, row, x_sem, to_y).wait_recv()
        elif name == "AGZ":
            tok_copy(j, row, p, zs.at[slot, r, p], target).start()
        elif name == "AGZM":
            meta_copy(j, row, zs.at[slot, r, pieces], target).start()
        elif name == "AGY":
            tok_copy(j, y, p, ys.at[j, p], to_y).start()
        elif name == "AGYM":
            meta_copy(j, y, ys.at[j, pieces], to_y).start()
        elif name == "NEAR":
            near_copy(j, part.at[j, other], p).start()
        elif name == "W0":
            local[0].wait()
            swapped[0].wait_recv()
        elif name == "W1":
            local[1].wait()
            swapped[1].wait_recv()
        elif name == "DZ":
            tok_copy(j, row, p, zs.at[slot, r, p], to_y).wait_send()
        elif name == "DZM":
            meta_copy(j, row, zs.at[slot, r, pieces], to_y).wait_send()
        elif name == "DY":
            tok_copy(j, y, p, ys.at[j, p], to_y).wait_send()
        elif name == "DYM":
            meta_copy(j, y, ys.at[j, pieces], to_y).wait_send()
        elif name == "DN_S":
            near_copy(j, part.at[j, other], p).wait_send()
        elif name == "DC":
            chain_copy(j, row, p, slot, to_y).wait_send()
        elif name == "OWN":
            own_copy.wait()

    def branch(m, program, low, high):
        if high - low == 1:
            for fields in program[low][0]:
                light(fields)
            return jnp.int32(packed(program[low][1]))
        half = (low + high) // 2
        return lax.cond(
            m < half, lambda: branch(m, program, low, half), lambda: branch(m, program, half, high)
        )

    def place(m, low, high):
        if high - low == 1:
            return branch(m, programs[low], 0, len(programs[low]))
        half = (low + high) // 2
        return lax.cond(z < half, lambda: place(m, low, half), lambda: place(m, half, high))

    def step(m, carry):
        word = place(m, 0, line)
        fields = []
        for size, _ in FIELDS:
            fields.append(lax.rem(word, jnp.int32(size)))
            word = lax.div(word, jnp.int32(size))
        op, j, r, p, dest, slot, f_near, f_below, f_above = fields
        row = jnp.where(r == 0, y, other)
        pl.when(op == HEAVY["UP"])(lambda: up(j, p))
        pl.when(op == HEAVY["HID"])(lambda: hidden(j))
        pl.when(op == HEAVY["DN"])(lambda: down(j, p))
        pl.when(op == HEAVY["SUM"])(lambda: sums(j, row, p, dest, slot, f_near, f_below, f_above))
        return carry

    lax.fori_loop(0, len(programs[0]), step, 0)
    for copy in swapped:
        copy.wait_send()


def on_grid(line, tokens, expert_ids, gate_weights, gate_up_weight, down_weight):
    experts = lax.axis_size("ep") * lax.axis_size("node")
    rows, width = tokens.shape
    inner = down_weight.shape[1]
    pieces = pieces_of(width)
    ag, rs = splits(line, pieces)
    order = plan(line, pieces, ag, rs, **dict(STYLE, tweak=mirrored(line, SHIFTS)))[0]
    programs = steps_of(line, pieces, ag, rs, order)
    dma, vmem, bf = pltpu.SemaphoreType.DMA, pltpu.VMEM, jnp.bfloat16
    return pl.pallas_call(
        functools.partial(kernel, line, pieces, experts, programs),
        out_shape=jax.ShapeDtypeStruct((rows, width), bf),
        in_specs=[
            pl.BlockSpec(memory_space=pltpu.VMEM),
            pl.BlockSpec(memory_space=pltpu.VMEM),
            pl.BlockSpec(memory_space=pl.ANY),
            pl.BlockSpec(memory_space=pl.ANY),
            pl.BlockSpec(memory_space=pl.ANY),
        ],
        out_specs=pl.BlockSpec(memory_space=pltpu.VMEM),
        scratch_shapes=[
            vmem((line, PAIR, rows, width), bf),
            vmem((line, PAIR, rows, LANES), bf),
            vmem((line, PAIR, rows, width), bf),
            vmem((line, rows, width), bf),
            vmem((line + 1, PAIR, rows, width), bf),
            vmem((2, width, 2 * inner), bf),
            vmem((2, inner, width), bf),
            vmem((line, 2, PAIR * rows, 2 * inner), jnp.float32),
            vmem((line, 2, PAIR * rows, inner), bf),
            vmem((line, 2, PAIR * rows, LANES), jnp.float32),
            vmem((rows, width // pieces), jnp.float32),
            dma(()), dma((2,)), dma((2,)), dma((2,)),
            dma((line, PAIR, pieces + 1)), dma((line + 1, PAIR, pieces + 1)),
            dma((line, pieces + 1)), dma((line, pieces)), dma((line, pieces)),
            dma((line + 1, PAIR, pieces)), dma((line, PAIR, pieces)),
        ],
        compiler_params=pltpu.CompilerParams(
            collective_id=0, has_side_effects=True, vmem_limit_bytes=VMEM_BYTES
        ),
    )(expert_ids.T, gate_weights.T, tokens, gate_up_weight, down_weight)


def on_device(tokens, expert_ids, gate_weights, gate_up_weight, down_weight):
    chips, cores = lax.axis_size("ep"), lax.axis_size("node")
    line = chips // PAIR
    rows, width = tokens.shape
    inner = down_weight.shape[1]
    planes = (6 * line + 3 * PAIR) * rows * width * 2 + 6 * inner * width * 2 * 1.1
    args = (tokens, expert_ids, gate_weights, gate_up_weight, down_weight)
    fits = planes < 0.9 * VMEM_BYTES and gate_up_weight.shape[0] == 1
    fits = fits and 2 * chips * cores <= LANES and pieces_of(width) > 1
    paired = cores == 2 and lax.axis_size("groups") * PAIR == 4
    if fits and paired and chips % PAIR == 0 and 1 < line < 9:
        return on_grid(line, *args)
    return spread_out(*args)


def solution(mesh):
    placed = (
        P(("groups", "ep", "node"), None),
        P(("groups", "ep", "node"), None),
        P(("groups", "ep", "node"), None),
        P(("ep", "node"), None, None),
        P(("ep", "node"), None, None),
    )
    return jax.shard_map(
        on_device,
        mesh=mesh,
        in_specs=placed,
        out_specs=P(("groups", "ep", "node"), None),
        check_vma=False,
    )
```

```python
import functools

import jax
import jax.numpy as jnp
from jax import lax
from jax.experimental import pallas as pl
from jax.experimental.pallas import tpu as pltpu
from jax.sharding import PartitionSpec as P

AXES = ("ep", "node")
DRAIN_AFTER = 8.0


def spread_out(tokens, expert_ids, gate_weights, gate_up_weight, down_weight):
    local_count, inner_width = down_weight.shape[0], down_weight.shape[1]
    device = lax.axis_index("ep") * lax.axis_size("node") + lax.axis_index("node")
    all_tokens = lax.all_gather(tokens, AXES, axis=0, tiled=True)
    all_ids = lax.all_gather(expert_ids, AXES, axis=0, tiled=True)
    all_weights = lax.all_gather(gate_weights, AXES, axis=0, tiled=True)
    total = 0.0
    for local in range(local_count):
        expert = device * local_count + local
        share = jnp.sum(jnp.where(all_ids == expert, all_weights, 0.0), axis=1)
        gate_up = jnp.dot(all_tokens, gate_up_weight[local], preferred_element_type=jnp.float32)
        hidden = (jax.nn.silu(gate_up[:, :inner_width]) * gate_up[:, inner_width:]).astype(
            jnp.bfloat16
        )
        product = jnp.dot(hidden, down_weight[local], preferred_element_type=jnp.float32)
        total = total + share[:, None] * product
    return lax.psum_scatter(total.astype(jnp.bfloat16), AXES, scatter_dimension=0, tiled=True)


SUB = 0.3
RATE = dict(z=1.284, y=1.284, lat=1.9, up=0.74, dn=0.63, up2=0.85, dn2=0.8, hid=0.45, sum=0.15, op=0.05, w0=11.0, w1=17.0, depth=1.5, meta=0.15)

def rank(style, b, top):
    if style == 'near': return b
    if style == 'far': return top - b
    return 0 if b == 0 else top + 1 - b

def plan(line, halves, pieces, ag, rs, style='nf', cstyle='nf', rate=None, sidefirst=True, own=1.5, tweak=None):
    R = dict(RATE); R.update(rate or {})
    L, P, H = line, pieces, halves
    B = L * H
    META = P
    time_of, waiting, avail, link, clock = {}, {}, [[] for _ in range(L)], {}, [0.0]*L
    order = [[] for _ in range(L)]
    count = 0
    def post(event, t):
        time_of[event] = t
        for op in waiting.pop(event, ()):
            op['need'] -= 1
            op['ready'] = max(op['ready'], t)
            if op['need'] == 0: avail[op['z']].append(op)
    ops = []
    def add(z, name, deps, key, lk=None):
        g = (z, name[0], name[1], name[4] if name[0] == 'AGZ' else '')
        if tweak: key = (key[0] * 100 + key[1] * 10 + tweak.get(g, 0),) + key[2:]
        op = dict(z=z, name=name, need=0, ready=0.0, key=key, link=lk)
        for d in set(deps):
            waiting.setdefault(d, []).append(op); op['need'] += 1
        ops.append(op)
        if op['need'] == 0: avail[z].append(op)
        return op
    sf = (lambda p: -p) if sidefirst else (lambda p: p)
    for z in range(L):
        for b in range(B):
            j, h = b // H, b % H
            d = abs(j - z)
            crank = (rank(cstyle, d-1, L-2) if d else own) + h * SUB
            for lk, step, ends in (('u', 1, L-1), ('d', -1, 0)):
                if z == ends or (j - z)*step > 0: continue
                a = rank(style, d, z if step > 0 else L-1-z) + h * SUB
                for p in list(range(P)) + [META]:
                    for r in ((0,) if p < ag[b] else (0, 1)):
                        add(z, ('AGZ', b, r, p, lk), [('t', z, b, r, p)], (0, a, p != META, sf(p), r), lk)
            for p in list(range(P)) + [META]:
                if p < ag[b] or j == z:
                    add(z, ('AGY', b, 0, p), [('t', z, b, 0, p)], (0, crank if j != z else -1 + h * SUB, p != META, sf(p)), 'y')
            for p in range(P):
                add(z, ('UP', b, p), [('t', z, b, 0, p), ('t', z, b, 1, p), ('w0', z)], (3, crank, sf(p)))
                add(z, ('DN', b, p), [('h', z, b), ('w1', z)], (2, crank, sf(p)))
            add(z, ('HID', b), [('a', z, b, p) for p in range(P)] + [('t', z, b, 0, META), ('t', z, b, 1, META)], (2, crank, -99))
            for p in range(rs[b]):
                add(z, ('NEAR', b, p), [('p', z, b, p)], (1, crank, sf(p)), 'y')
            for p in range(P):
                main = p < rs[b]
                for r in ((0,) if main else (1, 0)):
                    deps = [('p', z, b, p)]
                    if j == z:
                        if z > 0: deps.append(('c', z, b, r, p))
                        if z < L-1: deps.append(('c', z, B + h, r, p))
                        if r == 0: deps.append(('n', z, b, p))
                        add(z, ('FIN', b, r, p), deps, (1, -1 if r == 1 else 9, sf(p)), 'y' if r == 1 else None)
                    else:
                        if main: deps.append(('n', z, b, p))
                        if z > 0 if j > z else z < L-1: deps.append(('c', z, b, r, p))
                        add(z, ('SUM', b, r, p), deps, (1, crank, sf(p), -r), 'u' if j > z else 'd')
    for z in range(L):
        for lk in 'udy': link[z, lk] = 0.0
        for h in range(H):
            for p in range(P+1): post(('t', z, z*H + h, 0, p), 0.0)
        post(('w0', z), R['w0']); post(('w1', z), R['w1'])
    def send(z, lk, t, size):
        e = max(t, link[z, lk]) + size
        link[z, lk] = e
        return e + R['lat']
    left = len(ops)
    while left:
        best = None
        for z in range(L):
            if not avail[z]: continue
            st = min(max(o['ready'], link[z, o['link']] - R['depth']) if o['link'] else o['ready'] for o in avail[z])
            st = max(st, clock[z])
            if best is None or st < best[0]: best = (st, z)
        t, z = best
        cand = [o for o in avail[z] if o['ready'] <= t + 1e-9 and (not o['link'] or link[z, o['link']] - R['depth'] <= t + 1e-9)]
        op = min(cand, key=lambda o: o['key'])
        avail[z].remove(op)
        left -= 1
        n = op['name']; k = n[0]
        if k in ('AGZ', 'AGY'):
            te = t + R['op']
            size = R['meta'] if n[3] == META else R['y' if k == 'AGY' else 'z']
            if k == 'AGY': te2 = send(z, 'y', te, size); post(('t', z, n[1], 1, n[3]), te2)
            else:
                te2 = send(z, n[4], te, size)
                post(('t', z + (1 if n[4] == 'u' else -1), n[1], n[2], n[3]), te2)
        elif k in ('UP', 'DN'):
            done, made = ('a', 'up') if k == 'UP' else ('p', 'dn')
            group = [op] + [o for o in cand if H == 2 and o['name'] == (k, n[1] ^ 1, n[2])]
            te = t + R[made + ('2' if len(group) == 2 else '')]
            for o in group:
                post((done, z) + o['name'][1:], te)
            if len(group) == 2:
                avail[z].remove(group[1])
                left -= 1
                n = (k + '2', n[1] & ~1, n[2])
        elif k == 'HID':
            te = t + R['hid']; post(('h', z, n[1]), te)
        elif k == 'NEAR':
            te = t + R['op']; post(('n', z, n[1], n[2]), send(z, 'y', te, R['y']))
        elif k == 'SUM':
            te = t + R['sum']; j = n[1] // H; up = j > z; zz = z + (1 if up else -1)
            slot = B + n[1] % H if (zz == j and not up) else n[1]
            post(('c', zz, slot, n[2], n[3]), send(z, 'u' if up else 'd', te, R['z']))
        elif k == 'FIN':
            te = t + R['sum']
            if n[2] == 1: post(('n', z, n[1], n[3]), send(z, 'y', te, R['y']))
        clock[z] = te
        order[z].append((t, te, n))
    return order, max(clock), link


HALVES = 2
MOST = 4
AG, RS = (0.25, 0.75, 0.5, 0.5, 0.5, 0.5, 0.25, 0.75), (1.0, 0.5, 0.5, 1.0, 0.5, 1.0, 1.0, 0.5)
SHIFTS = {
    (0, 'AGY', 1, ''): -108.0, (0, 'AGY', 7, ''): -69.0, (0, 'HID', 6, ''): 30.0,
    (0, 'NEAR', 2, ''): -139.0, (0, 'UP', 0, ''): -131.0, (0, 'UP', 2, ''): -40.0,
    (0, 'UP', 7, ''): -45.0, (1, 'AGY', 0, ''): -116.0, (1, 'AGY', 1, ''): -148.0,
    (1, 'AGY', 3, ''): 21.0, (1, 'AGZ', 3, 'd'): 11.0, (1, 'AGZ', 3, 'u'): -44.0,
    (1, 'AGZ', 5, 'd'): 13.0, (1, 'DN', 3, ''): 102.0, (1, 'HID', 0, ''): 86.0,
    (1, 'HID', 5, ''): -129.0, (1, 'NEAR', 3, ''): -85.0, (1, 'SUM', 0, ''): -69.0,
    (1, 'SUM', 4, ''): -42.0, (1, 'UP', 0, ''): -75.0, (1, 'UP', 1, ''): 66.0,
    (1, 'UP', 3, ''): 39.0, (1, 'UP', 7, ''): -61.0,
}
STYLE = dict(style='far', cstyle='far', rate=dict(depth=1.2), sidefirst=False, own=1.5, tweak=None)


def mirrored(line, halves, shifts):
    turned = {"u": "d", "d": "u"}
    both = dict(shifts)
    for (z, name, b, way), value in shifts.items():
        other = (line - 1 - b // halves) * halves + b % halves
        both[line - 1 - z, name, other, turned.get(way, way)] = value
    return both


def pieces_of(width):
    return max(n for n in range(1, MOST + 1) if width % (n * LANES) == 0)


def splits(blocks, halves, pieces):
    last = len(AG) - 1
    return tuple(tuple(round(pieces * part[min(b, last)]) for b in range(blocks)) for part in (AG, RS))


PAIR = 2
LANES = 128
VMEM_BYTES = 55_900_000
MESH = pl.DeviceIdType.MESH
HEAVY = {"NONE": 0, "UP": 1, "HID": 2, "DN": 3, "SUM": 4, "UP2": 5, "DN2": 6}
UP_TO, DOWN_TO, SIDE_TO, HERE = 0, 1, 2, 3


def steps_of(line, halves, pieces, ag, rs, order):
    programs = []
    for z in range(line):
        steps, seen, drains = [], set(), []

        def emit(op, j=0, r=0, p=0, dest=0, slot=0, near=0, below=0, above=0):
            steps.append((op, j, r, p, dest, slot, near, below, above))

        def drain(t, *step):
            drains.append((t, step))

        def need(j, r, p):
            if (j, r, p) in seen:
                return
            seen.add((j, r, p))
            if j // halves == z and r == 0:
                if "own" not in seen:
                    seen.add("own")
                    emit("OWN")
            elif p == pieces:
                emit("RTM", j, r)
            else:
                emit("RT", j, r, p)

        def weight(which):
            if which not in seen:
                seen.add(which)
                emit(which)

        for start, end, n in order[z]:
            while drains and drains[0][0] < start - DRAIN_AFTER:
                emit(*drains.pop(0)[1])
            k = n[0]
            if k == "AGZ":
                _, j, r, p, lk = n
                need(j, r, p)
                dest = UP_TO if lk == "u" else DOWN_TO
                slot = j if j // halves != z or dest == UP_TO else line * halves + j % halves
                if p == pieces:
                    emit("AGZM", j, r, 0, dest, slot)
                    drain(start, "DZM", j, r, 0, dest, slot)
                else:
                    emit("AGZ", j, r, p, dest, slot)
                    drain(start, "DZ", j, r, p, dest, slot)
            elif k == "AGY":
                _, j, r, p = n
                need(j, r, p)
                if p == pieces:
                    emit("AGYM", j)
                    drain(start, "DYM", j)
                else:
                    emit("AGY", j, 0, p)
                    drain(start, "DY", j, 0, p)
            elif k == "UP":
                need(n[1], 0, n[2])
                need(n[1], 1, n[2])
                weight("W0")
                emit("UP", n[1], 0, n[2])
            elif k == "UP2":
                for half in range(2):
                    need(n[1] + half, 0, n[2])
                    need(n[1] + half, 1, n[2])
                weight("W0")
                emit("UP2", n[1], 0, n[2])
            elif k == "HID":
                need(n[1], 0, pieces)
                need(n[1], 1, pieces)
                emit("HID", n[1])
            elif k in ("DN", "DN2"):
                weight("W1")
                emit(k, n[1], 0, n[2])
            elif k == "NEAR":
                emit("NEAR", n[1], 0, n[2])
                drain(start, "DN_S", n[1], 0, n[2])
            elif k == "SUM":
                _, j, r, p = n
                up = j // halves > z
                far = j // halves == z - 1
                came = z > 0 if up else z < line - 1
                dest = UP_TO if up else DOWN_TO
                slot = line * halves + j % halves if far else j
                emit("SUM", j, r, p, dest, slot, int(p < rs[j]), int(came))
                drain(start, "DC", j, r, p, dest, slot)
            elif k == "FIN":
                _, j, r, p = n
                dest = SIDE_TO if r == 1 else HERE
                emit("SUM", j, r, p, dest, j, int(r == 0), int(z > 0), int(z < line - 1))
                if r == 1:
                    drain(start, "DN_S", j, 0, p)
        for _, step in drains:
            emit(*step)
        programs.append(grouped(steps))
    longest = max(len(p) for p in programs)
    return [p + [([], ("NONE",))] * (longest - len(p)) for p in programs]


def grouped(steps):
    groups, light = [], []
    for fields in steps:
        if fields[0] in HEAVY:
            groups.append((light, fields))
            light = []
        else:
            light.append(fields)
    return groups + [(light, ("NONE",))]


FIELDS = ((8, "op"), (16, "j"), (2, "r"), (32, "p"), (4, "dest"), (16, "slot"), (2, "near"), (2, "below"), (2, "above"))


def packed(step):
    word, scale = 0, 1
    for (size, _), value in zip(FIELDS, (HEAVY[step[0]],) + tuple(step[1:])):
        word += value * scale
        scale *= size
    return word


def kernel(
    line, halves, pieces, experts, programs, ids_ref, gate_ref, x_hbm, wgu_hbm, wd_hbm, out_ref,
    tok, meta, part, near, chain, wg, wd, acc, hid, share, tot,
    x_sem, w_l, w_s, w_r, tok_r, zs, ys, near_r, near_s, chain_r, chain_s,
):
    rows, width = out_ref.shape
    part_rows = rows // halves
    inner = wd.shape[1]
    block = width // pieces
    e = lax.axis_index("ep")
    c = lax.axis_index("node")
    z, y = e // PAIR, e % PAIR
    other = 1 - y
    has_dn, has_up = z > 0, z < line - 1
    to_up, to_dn = {"ep": e + PAIR}, {"ep": e - PAIR}
    to_y, to_core = {"ep": z * PAIR + other}, {"node": 1 - c}

    own_copies = [
        pltpu.make_async_copy(
            x_hbm.at[pl.ds(h * part_rows, part_rows)], tok.at[z * halves + h, y], x_sem.at[h]
        )
        for h in range(halves)
    ]
    for copy in own_copies:
        copy.start()
    local = [
        pltpu.make_async_copy(wgu_hbm.at[0], wg.at[0], w_l.at[0]),
        pltpu.make_async_copy(wd_hbm.at[0], wd.at[0], w_l.at[1]),
    ]
    for copy in local:
        copy.start()

    barrier = pltpu.get_barrier_semaphore()

    def greet(target):
        pl.semaphore_signal(barrier, inc=1, device_id=target, device_id_type=MESH)

    greet(to_core)
    greet(to_y)
    pl.when(has_up)(lambda: greet(to_up))
    pl.when(has_dn)(lambda: greet(to_dn))

    at_row = lax.broadcasted_iota(jnp.int32, (LANES, rows), 0)
    name = jnp.where(at_row < experts, at_row, at_row - experts)
    total = jnp.zeros((LANES, rows), jnp.float32)
    for k in range(ids_ref.shape[0]):
        total += jnp.where(ids_ref[k : k + 1, :] == name, gate_ref[k : k + 1, :], 0.0)
    high = total.astype(jnp.bfloat16).astype(jnp.float32)
    wide = jnp.where(at_row < experts, high, total - high)
    wide = jnp.where(at_row < 2 * experts, wide, 0.0).T.astype(jnp.bfloat16)
    for h in range(halves):
        meta[z * halves + h, y] = wide[h * part_rows : (h + 1) * part_rows]
    acc[...] = jnp.zeros_like(acc)

    pl.semaphore_wait(barrier, 2 + jnp.where(has_up, 1, 0) + jnp.where(has_dn, 1, 0))

    def remote(src, dst, s, r, target):
        return pltpu.make_async_remote_copy(
            src_ref=src, dst_ref=dst, send_sem=s, recv_sem=r,
            device_id=target, device_id_type=MESH,
        )

    swapped = [
        remote(wgu_hbm.at[0], wg.at[1], w_s.at[0], w_r.at[0], to_core),
        remote(wd_hbm.at[0], wd.at[1], w_s.at[1], w_r.at[1], to_core),
    ]
    for copy in swapped:
        copy.start()
    mine = e * 2 + c
    names = (mine, e * 2 + 1 - c)

    def span(p):
        return pl.ds(pl.multiple_of(p * block, LANES), block)

    def tok_copy(j, row, p, s, target):
        ref = tok.at[j, row, :, span(p)]
        return remote(ref, ref, s, tok_r.at[j, row, p], target)

    def meta_copy(j, row, s, target):
        ref = meta.at[j, row]
        return remote(ref, ref, s, tok_r.at[j, row, pieces], target)

    def both_ways(dest, act):
        pl.when(dest == UP_TO)(lambda: act(to_up))
        pl.when(dest == DOWN_TO)(lambda: act(to_dn))

    def near_copy(j, src, p):
        return remote(
            src.at[:, span(p)], near.at[j, :, span(p)], near_s.at[j, p], near_r.at[j, p], to_y
        )

    def chain_copy(j, row, p, slot, target):
        return remote(
            part.at[j, row, :, span(p)], chain.at[slot, row, :, span(p)],
            chain_s.at[j, row, p], chain_r.at[slot, row, p], target,
        )

    def up(j, p):
        at = span(p)
        rows_in = tok[j, :, :, at].reshape(PAIR * part_rows, block)
        for s in range(2):
            acc[j, s] += jnp.dot(rows_in, wg[s, at, :], preferred_element_type=jnp.float32)

    def up_two(j, p):
        at = span(p)
        count = PAIR * part_rows
        rows_in = tok[pl.ds(j, 2), :, :, at].reshape(2 * count, block)
        for s in range(2):
            both = jnp.dot(rows_in, wg[s, at, :], preferred_element_type=jnp.float32)
            acc[j, s] += both[:count]
            acc[j + 1, s] += both[count:]

    def down_two(j, p):
        at = span(p)
        count = PAIR * part_rows
        total = 0.0
        for s in range(2):
            both = jnp.concatenate([hid[j, s], hid[j + 1, s]])
            product = jnp.dot(both, wd[s, :, at], preferred_element_type=jnp.float32)
            total += jnp.concatenate([share[j, s, :, :1], share[j + 1, s, :, :1]]) * product
        part[pl.ds(j, 2), :, :, at] = total.astype(jnp.bfloat16).reshape(2, PAIR, part_rows, block)

    def hidden(j):
        for s in range(2):
            gate, over = acc[j, s, :, :inner], acc[j, s, :, inner:]
            hid[j, s] = (jax.nn.silu(gate) * over).astype(jnp.bfloat16)
        parts = meta[j].astype(jnp.float32).reshape(PAIR * part_rows, LANES)
        at = lax.broadcasted_iota(jnp.int32, parts.shape, 1)
        for s, expert in enumerate(names):
            kept = jnp.where((at == expert) | (at == expert + experts), parts, 0.0)
            share[j, s] = jnp.broadcast_to(
                jnp.sum(kept, axis=1, keepdims=True), (PAIR * part_rows, LANES)
            )

    def down(j, p):
        at = span(p)
        total = 0.0
        for s in range(2):
            product = jnp.dot(hid[j, s], wd[s, :, at], preferred_element_type=jnp.float32)
            total += share[j, s, :, :1] * product
        part[j, :, :, at] = total.astype(jnp.bfloat16).reshape(PAIR, part_rows, block)

    def sums(j, row, p, dest, slot, f_near, f_below, f_above):
        at = span(p)
        half = lax.rem(j, jnp.int32(halves))
        over = line * halves + half
        tot[...] = part[j, row, :, at].astype(jnp.float32)

        @pl.when(f_near == 1)
        def _():
            near_copy(j, part.at[j, row], p).wait_recv()
            tot[...] += near[j, :, at].astype(jnp.float32)

        @pl.when(f_below == 1)
        def _():
            chain_copy(j, row, p, j, to_y).wait_recv()
            tot[...] += chain[j, row, :, at].astype(jnp.float32)

        @pl.when(f_above == 1)
        def _():
            chain_copy(j, row, p, over, to_y).wait_recv()
            tot[...] += chain[over, row, :, at].astype(jnp.float32)

        value = tot[...].astype(jnp.bfloat16)

        @pl.when(dest == HERE)
        def _():
            out_ref[pl.ds(pl.multiple_of(half * part_rows, part_rows), part_rows), at] = value

        @pl.when(dest != HERE)
        def _():
            part[j, row, :, at] = value
            both_ways(dest, lambda target: chain_copy(j, row, p, slot, target).start())
            pl.when(dest == SIDE_TO)(lambda: near_copy(j, part.at[j, row], p).start())

    def light(fields):
        name, j, r, p, dest, slot = fields[:6]
        row = other if r else y
        target = to_up if dest == UP_TO else to_dn
        if name == "RT":
            tok_copy(j, row, p, x_sem.at[0], to_y).wait_recv()
        elif name == "RTM":
            meta_copy(j, row, x_sem.at[0], to_y).wait_recv()
        elif name == "AGZ":
            tok_copy(j, row, p, zs.at[slot, r, p], target).start()
        elif name == "AGZM":
            meta_copy(j, row, zs.at[slot, r, pieces], target).start()
        elif name == "AGY":
            tok_copy(j, y, p, ys.at[j, p], to_y).start()
        elif name == "AGYM":
            meta_copy(j, y, ys.at[j, pieces], to_y).start()
        elif name == "NEAR":
            near_copy(j, part.at[j, other], p).start()
        elif name == "W0":
            local[0].wait()
            swapped[0].wait_recv()
        elif name == "W1":
            local[1].wait()
            swapped[1].wait_recv()
        elif name == "DZ":
            tok_copy(j, row, p, zs.at[slot, r, p], to_y).wait_send()
        elif name == "DZM":
            meta_copy(j, row, zs.at[slot, r, pieces], to_y).wait_send()
        elif name == "DY":
            tok_copy(j, y, p, ys.at[j, p], to_y).wait_send()
        elif name == "DYM":
            meta_copy(j, y, ys.at[j, pieces], to_y).wait_send()
        elif name == "DN_S":
            near_copy(j, part.at[j, other], p).wait_send()
        elif name == "DC":
            chain_copy(j, row, p, slot, to_y).wait_send()
        elif name == "OWN":
            for copy in own_copies:
                copy.wait()

    def branch(m, program, low, high):
        if high - low == 1:
            for fields in program[low][0]:
                light(fields)
            return jnp.int32(packed(program[low][1]))
        half = (low + high) // 2
        return lax.cond(
            m < half, lambda: branch(m, program, low, half), lambda: branch(m, program, half, high)
        )

    def place(m, low, high):
        if high - low == 1:
            return branch(m, programs[low], 0, len(programs[low]))
        half = (low + high) // 2
        return lax.cond(z < half, lambda: place(m, low, half), lambda: place(m, half, high))

    def step(m, carry):
        word = place(m, 0, line)
        fields = []
        for size, _ in FIELDS:
            fields.append(lax.rem(word, jnp.int32(size)))
            word = lax.div(word, jnp.int32(size))
        op, j, r, p, dest, slot, f_near, f_below, f_above = fields
        row = jnp.where(r == 0, y, other)
        pl.when(op == HEAVY["UP"])(lambda: up(j, p))
        pl.when(op == HEAVY["HID"])(lambda: hidden(j))
        pl.when(op == HEAVY["DN"])(lambda: down(j, p))
        if halves == 2:
            pl.when(op == HEAVY["UP2"])(lambda: up_two(j, p))
            pl.when(op == HEAVY["DN2"])(lambda: down_two(j, p))
        pl.when(op == HEAVY["SUM"])(lambda: sums(j, row, p, dest, slot, f_near, f_below, f_above))
        return carry

    lax.fori_loop(0, len(programs[0]), step, 0)
    for copy in swapped:
        copy.wait_send()


def on_grid(line, tokens, expert_ids, gate_weights, gate_up_weight, down_weight):
    experts = lax.axis_size("ep") * lax.axis_size("node")
    rows, width = tokens.shape
    inner = down_weight.shape[1]
    halves, pieces = HALVES, pieces_of(width)
    blocks, part_rows = line * halves, rows // halves
    ag, rs = splits(blocks, halves, pieces)
    style = dict(STYLE, tweak=mirrored(line, halves, SHIFTS))
    order = plan(line, halves, pieces, ag, rs, **style)[0]
    programs = steps_of(line, halves, pieces, ag, rs, order)
    dma, vmem, bf = pltpu.SemaphoreType.DMA, pltpu.VMEM, jnp.bfloat16
    return pl.pallas_call(
        functools.partial(kernel, line, halves, pieces, experts, programs),
        out_shape=jax.ShapeDtypeStruct((rows, width), bf),
        in_specs=[
            pl.BlockSpec(memory_space=pltpu.VMEM),
            pl.BlockSpec(memory_space=pltpu.VMEM),
            pl.BlockSpec(memory_space=pl.ANY),
            pl.BlockSpec(memory_space=pl.ANY),
            pl.BlockSpec(memory_space=pl.ANY),
        ],
        out_specs=pl.BlockSpec(memory_space=pltpu.VMEM),
        scratch_shapes=[
            vmem((blocks, PAIR, part_rows, width), bf),
            vmem((blocks, PAIR, part_rows, LANES), bf),
            vmem((blocks, PAIR, part_rows, width), bf),
            vmem((blocks, part_rows, width), bf),
            vmem((blocks + halves, PAIR, part_rows, width), bf),
            vmem((2, width, 2 * inner), bf),
            vmem((2, inner, width), bf),
            vmem((blocks, 2, PAIR * part_rows, 2 * inner), jnp.float32),
            vmem((blocks, 2, PAIR * part_rows, inner), bf),
            vmem((blocks, 2, PAIR * part_rows, LANES), jnp.float32),
            vmem((part_rows, width // pieces), jnp.float32),
            dma((halves,)), dma((2,)), dma((2,)), dma((2,)),
            dma((blocks, PAIR, pieces + 1)), dma((blocks + halves, PAIR, pieces + 1)),
            dma((blocks, pieces + 1)), dma((blocks, pieces)), dma((blocks, pieces)),
            dma((blocks + halves, PAIR, pieces)), dma((blocks, PAIR, pieces)),
        ],
        compiler_params=pltpu.CompilerParams(
            collective_id=0, has_side_effects=True, vmem_limit_bytes=VMEM_BYTES
        ),
    )(expert_ids.T, gate_weights.T, tokens, gate_up_weight, down_weight)


def on_device(tokens, expert_ids, gate_weights, gate_up_weight, down_weight):
    chips, cores = lax.axis_size("ep"), lax.axis_size("node")
    line = chips // PAIR
    rows, width = tokens.shape
    inner = down_weight.shape[1]
    planes = (6 * line + 3 * PAIR) * rows * width * 2 + 6 * inner * width * 2 * 1.1
    args = (tokens, expert_ids, gate_weights, gate_up_weight, down_weight)
    fits = planes < 0.9 * VMEM_BYTES and gate_up_weight.shape[0] == 1
    fits = fits and 2 * chips * cores <= LANES and pieces_of(width) > 1
    fits = fits and rows % (16 * HALVES) == 0 and line * HALVES < 12
    paired = cores == 2 and lax.axis_size("groups") * PAIR == 4
    if fits and paired and chips % PAIR == 0 and 1 < line < 9:
        return on_grid(line, *args)
    return spread_out(*args)


def solution(mesh):
    placed = (
        P(("groups", "ep", "node"), None),
        P(("groups", "ep", "node"), None),
        P(("groups", "ep", "node"), None),
        P(("ep", "node"), None, None),
        P(("ep", "node"), None, None),
    )
    return jax.shard_map(
        on_device,
        mesh=mesh,
        in_specs=placed,
        out_specs=P(("groups", "ep", "node"), None),
        check_vma=False,
    )
```

```python
import functools

import jax
import jax.numpy as jnp
from jax import lax
from jax.experimental import pallas as pl
from jax.experimental.pallas import tpu as pltpu
from jax.sharding import PartitionSpec as P

AXES = ("ep", "node")
DRAIN_AFTER = 8.0


def spread_out(tokens, expert_ids, gate_weights, gate_up_weight, down_weight):
    local_count, inner_width = down_weight.shape[0], down_weight.shape[1]
    device = lax.axis_index("ep") * lax.axis_size("node") + lax.axis_index("node")
    all_tokens = lax.all_gather(tokens, AXES, axis=0, tiled=True)
    all_ids = lax.all_gather(expert_ids, AXES, axis=0, tiled=True)
    all_weights = lax.all_gather(gate_weights, AXES, axis=0, tiled=True)
    total = 0.0
    for local in range(local_count):
        expert = device * local_count + local
        share = jnp.sum(jnp.where(all_ids == expert, all_weights, 0.0), axis=1)
        gate_up = jnp.dot(all_tokens, gate_up_weight[local], preferred_element_type=jnp.float32)
        hidden = (jax.nn.silu(gate_up[:, :inner_width]) * gate_up[:, inner_width:]).astype(
            jnp.bfloat16
        )
        product = jnp.dot(hidden, down_weight[local], preferred_element_type=jnp.float32)
        total = total + share[:, None] * product
    return lax.psum_scatter(total.astype(jnp.bfloat16), AXES, scatter_dimension=0, tiled=True)


SUB = 0.3
RATE = dict(z=1.284, y=1.284, lat=1.9, up=0.74, dn=0.63, up2=0.85, dn2=0.8, hid=0.45, sum=0.15, op=0.05, w0=11.0, w1=17.0, depth=1.5, meta=0.23)

def rank(style, b, top):
    if style == 'near': return b
    if style == 'far': return top - b
    return 0 if b == 0 else top + 1 - b

def plan(line, halves, pieces, ag, rs, style='nf', cstyle='nf', rate=None, sidefirst=True, own=1.5, tweak=None):
    R = dict(RATE); R.update(rate or {})
    L, P, H = line, pieces, halves
    B = L * H
    META = P
    time_of, waiting, avail, link, clock = {}, {}, [[] for _ in range(L)], {}, [0.0]*L
    order = [[] for _ in range(L)]
    count = 0
    def post(event, t):
        time_of[event] = t
        for op in waiting.pop(event, ()):
            op['need'] -= 1
            op['ready'] = max(op['ready'], t)
            if op['need'] == 0: avail[op['z']].append(op)
    ops = []
    def add(z, name, deps, key, lk=None):
        g = (z, name[0], name[1], name[4] if name[0] == 'AGZ' else '')
        if tweak: key = (key[0] * 100 + key[1] * 10 + tweak.get(g, 0),) + key[2:]
        op = dict(z=z, name=name, need=0, ready=0.0, key=key, link=lk)
        for d in set(deps):
            waiting.setdefault(d, []).append(op); op['need'] += 1
        ops.append(op)
        if op['need'] == 0: avail[z].append(op)
        return op
    sf = (lambda p: -p) if sidefirst else (lambda p: p)
    for z in range(L):
        for b in range(B):
            j, h = b // H, b % H
            d = abs(j - z)
            crank = (rank(cstyle, d-1, L-2) if d else own) + h * SUB
            for lk, step, ends in (('u', 1, L-1), ('d', -1, 0)):
                if z == ends or (j - z)*step > 0: continue
                a = rank(style, d, z if step > 0 else L-1-z) + h * SUB
                for p in list(range(P)) + [META] * (h == 0):
                    for r in ((0,) if p < ag[b] else (0, 1)):
                        add(z, ('AGZ', b, r, p, lk), [('t', z, b, r, p)], (0, a, p != META, sf(p), r), lk)
            for p in list(range(P)) + [META] * (h == 0):
                if p < ag[b] or j == z:
                    add(z, ('AGY', b, 0, p), [('t', z, b, 0, p)], (0, crank if j != z else -1 + h * SUB, p != META, sf(p)), 'y')
            for p in range(P):
                add(z, ('UP', b, p), [('t', z, b, 0, p), ('t', z, b, 1, p), ('w0', z)], (3, crank, sf(p)))
                add(z, ('DN', b, p), [('h', z, b), ('w1', z)], (2, crank, sf(p)))
            add(z, ('HID', b), [('a', z, b, p) for p in range(P)] + [('t', z, j*H, 0, META), ('t', z, j*H, 1, META)], (2, crank, -99))
            for p in range(rs[b]):
                add(z, ('NEAR', b, p), [('p', z, b, p)], (1, crank, sf(p)), 'y')
            for p in range(P):
                main = p < rs[b]
                for r in ((0,) if main else (1, 0)):
                    deps = [('p', z, b, p)]
                    if j == z:
                        if z > 0: deps.append(('c', z, b, r, p))
                        if z < L-1: deps.append(('c', z, B + h, r, p))
                        if r == 0: deps.append(('n', z, b, p))
                        add(z, ('FIN', b, r, p), deps, (1, -1 if r == 1 else 9, sf(p)), 'y' if r == 1 else None)
                    else:
                        if main: deps.append(('n', z, b, p))
                        if z > 0 if j > z else z < L-1: deps.append(('c', z, b, r, p))
                        add(z, ('SUM', b, r, p), deps, (1, crank, sf(p), -r), 'u' if j > z else 'd')
    for z in range(L):
        for lk in 'udy': link[z, lk] = 0.0
        for h in range(H):
            for p in range(P+1): post(('t', z, z*H + h, 0, p), 0.0)
        post(('w0', z), R['w0']); post(('w1', z), R['w1'])
    def send(z, lk, t, size):
        e = max(t, link[z, lk]) + size
        link[z, lk] = e
        return e + R['lat']
    left = len(ops)
    while left:
        best = None
        for z in range(L):
            if not avail[z]: continue
            st = min(max(o['ready'], link[z, o['link']] - R['depth']) if o['link'] else o['ready'] for o in avail[z])
            st = max(st, clock[z])
            if best is None or st < best[0]: best = (st, z)
        t, z = best
        cand = [o for o in avail[z] if o['ready'] <= t + 1e-9 and (not o['link'] or link[z, o['link']] - R['depth'] <= t + 1e-9)]
        op = min(cand, key=lambda o: o['key'])
        avail[z].remove(op)
        left -= 1
        n = op['name']; k = n[0]
        if k in ('AGZ', 'AGY'):
            te = t + R['op']
            size = R['meta'] if n[3] == META else R['y' if k == 'AGY' else 'z']
            if k == 'AGY': te2 = send(z, 'y', te, size); post(('t', z, n[1], 1, n[3]), te2)
            else:
                te2 = send(z, n[4], te, size)
                post(('t', z + (1 if n[4] == 'u' else -1), n[1], n[2], n[3]), te2)
        elif k in ('UP', 'DN'):
            done, made = ('a', 'up') if k == 'UP' else ('p', 'dn')
            group = [op] + [o for o in cand if H == 2 and o['name'] == (k, n[1] ^ 1, n[2])]
            te = t + R[made + ('2' if len(group) == 2 else '')]
            for o in group:
                post((done, z) + o['name'][1:], te)
            if len(group) == 2:
                avail[z].remove(group[1])
                left -= 1
                n = (k + '2', n[1] & ~1, n[2])
        elif k == 'HID':
            te = t + R['hid']; post(('h', z, n[1]), te)
        elif k == 'NEAR':
            te = t + R['op']; post(('n', z, n[1], n[2]), send(z, 'y', te, R['y']))
        elif k == 'SUM':
            te = t + R['sum']; j = n[1] // H; up = j > z; zz = z + (1 if up else -1)
            slot = B + n[1] % H if (zz == j and not up) else n[1]
            post(('c', zz, slot, n[2], n[3]), send(z, 'u' if up else 'd', te, R['z']))
        elif k == 'FIN':
            te = t + R['sum']
            if n[2] == 1: post(('n', z, n[1], n[3]), send(z, 'y', te, R['y']))
        clock[z] = te
        order[z].append((t, te, n))
    return order, max(clock), link


HALVES = 2
MOST = 4
AG, RS = (0.25, 0.75, 0.5, 0.5, 0.5, 0.5, 0.25, 0.75), (1.0, 0.5, 0.5, 1.0, 0.5, 1.0, 1.0, 0.5)
SHIFTS = {
    (0, 'AGY', 0, ''): 75.74, (0, 'AGY', 1, ''): -107.52, (0, 'AGY', 2, ''): 93.39,
    (0, 'AGY', 3, ''): 122.46, (0, 'AGY', 4, ''): -1.56, (0, 'AGY', 5, ''): -184.63,
    (0, 'AGY', 6, ''): -3.66, (0, 'AGY', 7, ''): -68.82, (0, 'AGZ', 0, 'd'): 10.21,
    (0, 'AGZ', 0, 'u'): 58.64, (0, 'AGZ', 1, 'd'): 90.19, (0, 'AGZ', 1, 'u'): 74.78,
    (0, 'AGZ', 2, 'd'): 83.79, (0, 'AGZ', 2, 'u'): 125.7, (0, 'AGZ', 3, 'd'): -5.37,
    (0, 'AGZ', 3, 'u'): -62.66, (0, 'AGZ', 4, 'd'): -158.02, (0, 'AGZ', 4, 'u'): -144.91,
    (0, 'AGZ', 5, 'd'): 66.06, (0, 'AGZ', 5, 'u'): 37.48, (0, 'AGZ', 6, 'd'): -126.18,
    (0, 'AGZ', 6, 'u'): -192.65, (0, 'AGZ', 7, 'd'): -31.03, (0, 'AGZ', 7, 'u'): -2.99,
    (0, 'DN', 0, ''): 30.47, (0, 'DN', 1, ''): 178.94, (0, 'DN', 2, ''): 10.51,
    (0, 'DN', 3, ''): 67.83, (0, 'DN', 4, ''): -35.99, (0, 'DN', 5, ''): 27.04,
    (0, 'DN', 6, ''): 23.23, (0, 'DN', 7, ''): -20.52, (0, 'FIN', 0, ''): -53.87,
    (0, 'FIN', 1, ''): 49.76, (0, 'FIN', 2, ''): -9.79, (0, 'FIN', 3, ''): 25.25,
    (0, 'FIN', 4, ''): -111.85, (0, 'FIN', 5, ''): -34.61, (0, 'FIN', 6, ''): 23.62,
    (0, 'FIN', 7, ''): 40.9, (0, 'HID', 0, ''): -10.3, (0, 'HID', 1, ''): -71.55,
    (0, 'HID', 2, ''): -46.61, (0, 'HID', 3, ''): 62.94, (0, 'HID', 4, ''): 23.54,
    (0, 'HID', 5, ''): 12.69, (0, 'HID', 6, ''): 30.34, (0, 'HID', 7, ''): -18.5,
    (0, 'NEAR', 0, ''): 33.99, (0, 'NEAR', 1, ''): 33.86, (0, 'NEAR', 2, ''): -138.54,
    (0, 'NEAR', 3, ''): -29.78, (0, 'NEAR', 4, ''): 49.06, (0, 'NEAR', 5, ''): 58.77,
    (0, 'NEAR', 6, ''): 86.66, (0, 'NEAR', 7, ''): 21.99, (0, 'SUM', 0, ''): -27.77,
    (0, 'SUM', 1, ''): 16.47, (0, 'SUM', 2, ''): 58.91, (0, 'SUM', 3, ''): -67.76,
    (0, 'SUM', 4, ''): -32.45, (0, 'SUM', 5, ''): 7.77, (0, 'SUM', 6, ''): -120.03,
    (0, 'SUM', 7, ''): 13.54, (0, 'UP', 0, ''): -130.65, (0, 'UP', 1, ''): 142.4,
    (0, 'UP', 2, ''): -40.31, (0, 'UP', 3, ''): -12.29, (0, 'UP', 4, ''): -68.57,
    (0, 'UP', 5, ''): 10.47, (0, 'UP', 6, ''): 7.16, (0, 'UP', 7, ''): -44.69,
    (1, 'AGY', 0, ''): -115.63, (1, 'AGY', 1, ''): -147.53, (1, 'AGY', 2, ''): -5.18,
    (1, 'AGY', 3, ''): 20.69, (1, 'AGY', 4, ''): 23.6, (1, 'AGY', 5, ''): 61.08,
    (1, 'AGY', 6, ''): -108.08, (1, 'AGY', 7, ''): -0.23, (1, 'AGZ', 0, 'd'): 84.61,
    (1, 'AGZ', 0, 'u'): -47.23, (1, 'AGZ', 1, 'd'): -110.73, (1, 'AGZ', 1, 'u'): -9.49,
    (1, 'AGZ', 2, 'd'): -5.64, (1, 'AGZ', 2, 'u'): 25.14, (1, 'AGZ', 3, 'd'): 10.69,
    (1, 'AGZ', 3, 'u'): -44.08, (1, 'AGZ', 4, 'd'): -34.64, (1, 'AGZ', 4, 'u'): 25.54,
    (1, 'AGZ', 5, 'd'): 12.74, (1, 'AGZ', 5, 'u'): 26.21, (1, 'AGZ', 6, 'd'): -30.75,
    (1, 'AGZ', 6, 'u'): 110.32, (1, 'AGZ', 7, 'd'): -37.55, (1, 'AGZ', 7, 'u'): -100.64,
    (1, 'DN', 0, ''): 5.73, (1, 'DN', 1, ''): -117.79, (1, 'DN', 2, ''): -122.16,
    (1, 'DN', 3, ''): 102.39, (1, 'DN', 4, ''): -19.51, (1, 'DN', 5, ''): 41.63,
    (1, 'DN', 6, ''): -61.83, (1, 'DN', 7, ''): 6.53, (1, 'FIN', 0, ''): 16.64,
    (1, 'FIN', 1, ''): 30.82, (1, 'FIN', 2, ''): -87.38, (1, 'FIN', 3, ''): 5.63,
    (1, 'FIN', 4, ''): 142.35, (1, 'FIN', 5, ''): 11.19, (1, 'FIN', 6, ''): -70.69,
    (1, 'FIN', 7, ''): -35.7, (1, 'HID', 0, ''): 86.41, (1, 'HID', 1, ''): -126.17,
    (1, 'HID', 2, ''): -25.6, (1, 'HID', 3, ''): -18.73, (1, 'HID', 4, ''): -13.15,
    (1, 'HID', 5, ''): -128.66, (1, 'HID', 6, ''): -46.31, (1, 'HID', 7, ''): 4.65,
    (1, 'NEAR', 0, ''): -67.58, (1, 'NEAR', 1, ''): 17.99, (1, 'NEAR', 2, ''): -39.22,
    (1, 'NEAR', 3, ''): -84.68, (1, 'NEAR', 4, ''): -43.47, (1, 'NEAR', 5, ''): 150.74,
    (1, 'NEAR', 6, ''): -24.69, (1, 'NEAR', 7, ''): -101.06, (1, 'SUM', 0, ''): -68.57,
    (1, 'SUM', 1, ''): 297.99, (1, 'SUM', 2, ''): 62.81, (1, 'SUM', 3, ''): 29.89,
    (1, 'SUM', 4, ''): -41.77, (1, 'SUM', 5, ''): 89.48, (1, 'SUM', 6, ''): -110.69,
    (1, 'SUM', 7, ''): -16.09, (1, 'UP', 0, ''): -75.26, (1, 'UP', 1, ''): 66.45,
    (1, 'UP', 2, ''): -48.19, (1, 'UP', 3, ''): 38.78, (1, 'UP', 4, ''): 16.03,
    (1, 'UP', 5, ''): 30.82, (1, 'UP', 6, ''): 3.65, (1, 'UP', 7, ''): -61.06,
}
STYLE = dict(style='far', cstyle='far', rate=dict(depth=1.2), sidefirst=False, own=1.5, tweak=None)


def mirrored(line, halves, shifts):
    turned = {"u": "d", "d": "u"}
    both = dict(shifts)
    for (z, name, b, way), value in shifts.items():
        other = (line - 1 - b // halves) * halves + b % halves
        both[line - 1 - z, name, other, turned.get(way, way)] = value
    return both


def pieces_of(width):
    return max(n for n in range(1, MOST + 1) if width % (n * LANES) == 0)


def splits(blocks, halves, pieces):
    last = len(AG) - 1
    return tuple(tuple(round(pieces * part[min(b, last)]) for b in range(blocks)) for part in (AG, RS))


PAIR = 2
LANES = 128
VMEM_BYTES = 55_900_000
MESH = pl.DeviceIdType.MESH
HEAVY = {"NONE": 0, "UP": 1, "HID": 2, "DN": 3, "SUM": 4, "UP2": 5, "DN2": 6}
UP_TO, DOWN_TO, SIDE_TO, HERE = 0, 1, 2, 3


def steps_of(line, halves, pieces, ag, rs, order):
    programs = []
    for z in range(line):
        steps, seen, drains = [], set(), []

        def emit(op, j=0, r=0, p=0, dest=0, slot=0, near=0, below=0, above=0):
            steps.append((op, j, r, p, dest, slot, near, below, above))

        def drain(t, *step):
            drains.append((t, step))

        def need(j, r, p):
            if (j, r, p) in seen:
                return
            seen.add((j, r, p))
            if j // halves == z and r == 0:
                if "own" not in seen:
                    seen.add("own")
                    emit("OWN")
            elif p == pieces:
                emit("RTM", j, r)
            else:
                emit("RT", j, r, p)

        def weight(which):
            if which not in seen:
                seen.add(which)
                emit(which)

        for start, end, n in order[z]:
            while drains and drains[0][0] < start - DRAIN_AFTER:
                emit(*drains.pop(0)[1])
            k = n[0]
            if k == "AGZ":
                _, j, r, p, lk = n
                need(j, r, p)
                dest = UP_TO if lk == "u" else DOWN_TO
                slot = j if j // halves != z or dest == UP_TO else line * halves + j % halves
                if p == pieces:
                    emit("AGZM", j, r, 0, dest, slot)
                    drain(start, "DZM", j, r, 0, dest, slot)
                else:
                    emit("AGZ", j, r, p, dest, slot)
                    drain(start, "DZ", j, r, p, dest, slot)
            elif k == "AGY":
                _, j, r, p = n
                need(j, r, p)
                if p == pieces:
                    emit("AGYM", j)
                    drain(start, "DYM", j)
                else:
                    emit("AGY", j, 0, p)
                    drain(start, "DY", j, 0, p)
            elif k == "UP":
                need(n[1], 0, n[2])
                need(n[1], 1, n[2])
                weight("W0")
                emit("UP", n[1], 0, n[2])
            elif k == "UP2":
                for half in range(2):
                    need(n[1] + half, 0, n[2])
                    need(n[1] + half, 1, n[2])
                weight("W0")
                emit("UP2", n[1], 0, n[2])
            elif k == "HID":
                need(n[1] // halves * halves, 0, pieces)
                need(n[1] // halves * halves, 1, pieces)
                emit("HID", n[1])
            elif k in ("DN", "DN2"):
                weight("W1")
                emit(k, n[1], 0, n[2])
            elif k == "NEAR":
                emit("NEAR", n[1], 0, n[2])
                drain(start, "DN_S", n[1], 0, n[2])
            elif k == "SUM":
                _, j, r, p = n
                up = j // halves > z
                far = j // halves == z - 1
                came = z > 0 if up else z < line - 1
                dest = UP_TO if up else DOWN_TO
                slot = line * halves + j % halves if far else j
                emit("SUM", j, r, p, dest, slot, int(p < rs[j]), int(came))
                drain(start, "DC", j, r, p, dest, slot)
            elif k == "FIN":
                _, j, r, p = n
                dest = SIDE_TO if r == 1 else HERE
                emit("SUM", j, r, p, dest, j, int(r == 0), int(z > 0), int(z < line - 1))
                if r == 1:
                    drain(start, "DN_S", j, 0, p)
        for _, step in drains:
            emit(*step)
        programs.append(grouped(steps))
    longest = max(len(p) for p in programs)
    return [p + [([], ("NONE",))] * (longest - len(p)) for p in programs]


def grouped(steps):
    groups, light = [], []
    for fields in steps:
        if fields[0] in HEAVY:
            groups.append((light, fields))
            light = []
        else:
            light.append(fields)
    return groups + [(light, ("NONE",))]


FIELDS = ((8, "op"), (16, "j"), (2, "r"), (32, "p"), (4, "dest"), (16, "slot"), (2, "near"), (2, "below"), (2, "above"))


def packed(step):
    word, scale = 0, 1
    for (size, _), value in zip(FIELDS, (HEAVY[step[0]],) + tuple(step[1:])):
        word += value * scale
        scale *= size
    return word


def kernel(
    line, halves, pieces, experts, programs, ids_ref, gate_ref, x_hbm, wgu_hbm, wd_hbm, out_ref,
    tok, meta, part, near, chain, wg, wd, acc, hid, share, tot,
    x_sem, w_l, w_s, w_r, tok_r, zs, ys, near_r, near_s, chain_r, chain_s,
):
    rows, width = out_ref.shape
    part_rows = rows // halves
    inner = wd.shape[1]
    block = width // pieces
    e = lax.axis_index("ep")
    c = lax.axis_index("node")
    z, y = e // PAIR, e % PAIR
    other = 1 - y
    has_dn, has_up = z > 0, z < line - 1
    to_up, to_dn = {"ep": e + PAIR}, {"ep": e - PAIR}
    to_y, to_core = {"ep": z * PAIR + other}, {"node": 1 - c}

    own_copies = [
        pltpu.make_async_copy(
            x_hbm.at[pl.ds(h * part_rows, part_rows)], tok.at[z * halves + h, y], x_sem.at[h]
        )
        for h in range(halves)
    ]
    for copy in own_copies:
        copy.start()
    local = [
        pltpu.make_async_copy(wgu_hbm.at[0], wg.at[0], w_l.at[0]),
        pltpu.make_async_copy(wd_hbm.at[0], wd.at[0], w_l.at[1]),
    ]
    for copy in local:
        copy.start()

    barrier = pltpu.get_barrier_semaphore()

    def greet(target):
        pl.semaphore_signal(barrier, inc=1, device_id=target, device_id_type=MESH)

    greet(to_core)
    greet(to_y)
    pl.when(has_up)(lambda: greet(to_up))
    pl.when(has_dn)(lambda: greet(to_dn))

    at_row = lax.broadcasted_iota(jnp.int32, (LANES, rows), 0)
    name = jnp.where(at_row < experts, at_row, at_row - experts)
    total = jnp.zeros((LANES, rows), jnp.float32)
    for k in range(ids_ref.shape[0]):
        total += jnp.where(ids_ref[k : k + 1, :] == name, gate_ref[k : k + 1, :], 0.0)
    high = total.astype(jnp.bfloat16).astype(jnp.float32)
    wide = jnp.where(at_row < experts, high, total - high)
    wide = jnp.where(at_row < 2 * experts, wide, 0.0).T.astype(jnp.bfloat16)
    for h in range(halves):
        meta[z * halves + h, y] = wide[h * part_rows : (h + 1) * part_rows]
    acc[...] = jnp.zeros_like(acc)

    pl.semaphore_wait(barrier, 2 + jnp.where(has_up, 1, 0) + jnp.where(has_dn, 1, 0))

    def remote(src, dst, s, r, target):
        return pltpu.make_async_remote_copy(
            src_ref=src, dst_ref=dst, send_sem=s, recv_sem=r,
            device_id=target, device_id_type=MESH,
        )

    swapped = [
        remote(wgu_hbm.at[0], wg.at[1], w_s.at[0], w_r.at[0], to_core),
        remote(wd_hbm.at[0], wd.at[1], w_s.at[1], w_r.at[1], to_core),
    ]
    for copy in swapped:
        copy.start()
    mine = e * 2 + c
    names = (mine, e * 2 + 1 - c)

    def span(p):
        return pl.ds(pl.multiple_of(p * block, LANES), block)

    def tok_copy(j, row, p, s, target):
        ref = tok.at[j, row, :, span(p)]
        return remote(ref, ref, s, tok_r.at[j, row, p], target)

    def meta_copy(j, row, s, target):
        ref = meta.at[pl.ds(j, halves), row]
        return remote(ref, ref, s, tok_r.at[j, row, pieces], target)

    def both_ways(dest, act):
        pl.when(dest == UP_TO)(lambda: act(to_up))
        pl.when(dest == DOWN_TO)(lambda: act(to_dn))

    def near_copy(j, src, p):
        return remote(
            src.at[:, span(p)], near.at[j, :, span(p)], near_s.at[j, p], near_r.at[j, p], to_y
        )

    def chain_copy(j, row, p, slot, target):
        return remote(
            part.at[j, row, :, span(p)], chain.at[slot, row, :, span(p)],
            chain_s.at[j, row, p], chain_r.at[slot, row, p], target,
        )

    def up(j, p):
        at = span(p)
        rows_in = tok[j, :, :, at].reshape(PAIR * part_rows, block)
        for s in range(2):
            acc[j, s] += jnp.dot(rows_in, wg[s, at, :], preferred_element_type=jnp.float32)

    def up_two(j, p):
        at = span(p)
        count = PAIR * part_rows
        rows_in = tok[pl.ds(j, 2), :, :, at].reshape(2 * count, block)
        for s in range(2):
            both = jnp.dot(rows_in, wg[s, at, :], preferred_element_type=jnp.float32)
            acc[j, s] += both[:count]
            acc[j + 1, s] += both[count:]

    def down_two(j, p):
        at = span(p)
        count = PAIR * part_rows
        total = 0.0
        for s in range(2):
            both = jnp.concatenate([hid[j, s], hid[j + 1, s]])
            product = jnp.dot(both, wd[s, :, at], preferred_element_type=jnp.float32)
            total += jnp.concatenate([share[j, s, :, :1], share[j + 1, s, :, :1]]) * product
        part[pl.ds(j, 2), :, :, at] = total.astype(jnp.bfloat16).reshape(2, PAIR, part_rows, block)

    def hidden(j):
        for s in range(2):
            gate, over = acc[j, s, :, :inner], acc[j, s, :, inner:]
            hid[j, s] = (jax.nn.silu(gate) * over).astype(jnp.bfloat16)
        parts = meta[j].astype(jnp.float32).reshape(PAIR * part_rows, LANES)
        at = lax.broadcasted_iota(jnp.int32, parts.shape, 1)
        for s, expert in enumerate(names):
            kept = jnp.where((at == expert) | (at == expert + experts), parts, 0.0)
            share[j, s] = jnp.broadcast_to(
                jnp.sum(kept, axis=1, keepdims=True), (PAIR * part_rows, LANES)
            )

    def down(j, p):
        at = span(p)
        total = 0.0
        for s in range(2):
            product = jnp.dot(hid[j, s], wd[s, :, at], preferred_element_type=jnp.float32)
            total += share[j, s, :, :1] * product
        part[j, :, :, at] = total.astype(jnp.bfloat16).reshape(PAIR, part_rows, block)

    def sums(j, row, p, dest, slot, f_near, f_below, f_above):
        at = span(p)
        half = lax.rem(j, jnp.int32(halves))
        over = line * halves + half
        tot[...] = part[j, row, :, at].astype(jnp.float32)

        @pl.when(f_near == 1)
        def _():
            near_copy(j, part.at[j, row], p).wait_recv()
            tot[...] += near[j, :, at].astype(jnp.float32)

        @pl.when(f_below == 1)
        def _():
            chain_copy(j, row, p, j, to_y).wait_recv()
            tot[...] += chain[j, row, :, at].astype(jnp.float32)

        @pl.when(f_above == 1)
        def _():
            chain_copy(j, row, p, over, to_y).wait_recv()
            tot[...] += chain[over, row, :, at].astype(jnp.float32)

        value = tot[...].astype(jnp.bfloat16)

        @pl.when(dest == HERE)
        def _():
            out_ref[pl.ds(pl.multiple_of(half * part_rows, part_rows), part_rows), at] = value

        @pl.when(dest != HERE)
        def _():
            part[j, row, :, at] = value
            both_ways(dest, lambda target: chain_copy(j, row, p, slot, target).start())
            pl.when(dest == SIDE_TO)(lambda: near_copy(j, part.at[j, row], p).start())

    def light(fields):
        name, j, r, p, dest, slot = fields[:6]
        row = other if r else y
        target = to_up if dest == UP_TO else to_dn
        if name == "RT":
            tok_copy(j, row, p, x_sem.at[0], to_y).wait_recv()
        elif name == "RTM":
            meta_copy(j, row, x_sem.at[0], to_y).wait_recv()
        elif name == "AGZ":
            tok_copy(j, row, p, zs.at[slot, r, p], target).start()
        elif name == "AGZM":
            meta_copy(j, row, zs.at[slot, r, pieces], target).start()
        elif name == "AGY":
            tok_copy(j, y, p, ys.at[j, p], to_y).start()
        elif name == "AGYM":
            meta_copy(j, y, ys.at[j, pieces], to_y).start()
        elif name == "NEAR":
            near_copy(j, part.at[j, other], p).start()
        elif name == "W0":
            local[0].wait()
            swapped[0].wait_recv()
        elif name == "W1":
            local[1].wait()
            swapped[1].wait_recv()
        elif name == "DZ":
            tok_copy(j, row, p, zs.at[slot, r, p], to_y).wait_send()
        elif name == "DZM":
            meta_copy(j, row, zs.at[slot, r, pieces], to_y).wait_send()
        elif name == "DY":
            tok_copy(j, y, p, ys.at[j, p], to_y).wait_send()
        elif name == "DYM":
            meta_copy(j, y, ys.at[j, pieces], to_y).wait_send()
        elif name == "DN_S":
            near_copy(j, part.at[j, other], p).wait_send()
        elif name == "DC":
            chain_copy(j, row, p, slot, to_y).wait_send()
        elif name == "OWN":
            for copy in own_copies:
                copy.wait()

    def branch(m, program, low, high):
        if high - low == 1:
            for fields in program[low][0]:
                light(fields)
            return jnp.int32(packed(program[low][1]))
        half = (low + high) // 2
        return lax.cond(
            m < half, lambda: branch(m, program, low, half), lambda: branch(m, program, half, high)
        )

    def place(m, low, high):
        if high - low == 1:
            return branch(m, programs[low], 0, len(programs[low]))
        half = (low + high) // 2
        return lax.cond(z < half, lambda: place(m, low, half), lambda: place(m, half, high))

    def step(m, carry):
        word = place(m, 0, line)
        fields = []
        for size, _ in FIELDS:
            fields.append(lax.rem(word, jnp.int32(size)))
            word = lax.div(word, jnp.int32(size))
        op, j, r, p, dest, slot, f_near, f_below, f_above = fields
        row = jnp.where(r == 0, y, other)
        pl.when(op == HEAVY["UP"])(lambda: up(j, p))
        pl.when(op == HEAVY["HID"])(lambda: hidden(j))
        pl.when(op == HEAVY["DN"])(lambda: down(j, p))
        if halves == 2:
            pl.when(op == HEAVY["UP2"])(lambda: up_two(j, p))
            pl.when(op == HEAVY["DN2"])(lambda: down_two(j, p))
        pl.when(op == HEAVY["SUM"])(lambda: sums(j, row, p, dest, slot, f_near, f_below, f_above))
        return carry

    lax.fori_loop(0, len(programs[0]), step, 0)
    for copy in swapped:
        copy.wait_send()


def on_grid(line, tokens, expert_ids, gate_weights, gate_up_weight, down_weight):
    experts = lax.axis_size("ep") * lax.axis_size("node")
    rows, width = tokens.shape
    inner = down_weight.shape[1]
    halves, pieces = HALVES, pieces_of(width)
    blocks, part_rows = line * halves, rows // halves
    ag, rs = splits(blocks, halves, pieces)
    style = dict(STYLE, tweak=mirrored(line, halves, SHIFTS))
    order = plan(line, halves, pieces, ag, rs, **style)[0]
    programs = steps_of(line, halves, pieces, ag, rs, order)
    dma, vmem, bf = pltpu.SemaphoreType.DMA, pltpu.VMEM, jnp.bfloat16
    return pl.pallas_call(
        functools.partial(kernel, line, halves, pieces, experts, programs),
        out_shape=jax.ShapeDtypeStruct((rows, width), bf),
        in_specs=[
            pl.BlockSpec(memory_space=pltpu.VMEM),
            pl.BlockSpec(memory_space=pltpu.VMEM),
            pl.BlockSpec(memory_space=pl.ANY),
            pl.BlockSpec(memory_space=pl.ANY),
            pl.BlockSpec(memory_space=pl.ANY),
        ],
        out_specs=pl.BlockSpec(memory_space=pltpu.VMEM),
        scratch_shapes=[
            vmem((blocks, PAIR, part_rows, width), bf),
            vmem((blocks, PAIR, part_rows, LANES), bf),
            vmem((blocks, PAIR, part_rows, width), bf),
            vmem((blocks, part_rows, width), bf),
            vmem((blocks + halves, PAIR, part_rows, width), bf),
            vmem((2, width, 2 * inner), bf),
            vmem((2, inner, width), bf),
            vmem((blocks, 2, PAIR * part_rows, 2 * inner), jnp.float32),
            vmem((blocks, 2, PAIR * part_rows, inner), bf),
            vmem((blocks, 2, PAIR * part_rows, LANES), jnp.float32),
            vmem((part_rows, width // pieces), jnp.float32),
            dma((halves,)), dma((2,)), dma((2,)), dma((2,)),
            dma((blocks, PAIR, pieces + 1)), dma((blocks + halves, PAIR, pieces + 1)),
            dma((blocks, pieces + 1)), dma((blocks, pieces)), dma((blocks, pieces)),
            dma((blocks + halves, PAIR, pieces)), dma((blocks, PAIR, pieces)),
        ],
        compiler_params=pltpu.CompilerParams(
            collective_id=0, has_side_effects=True, vmem_limit_bytes=VMEM_BYTES
        ),
    )(expert_ids.T, gate_weights.T, tokens, gate_up_weight, down_weight)


def on_device(tokens, expert_ids, gate_weights, gate_up_weight, down_weight):
    chips, cores = lax.axis_size("ep"), lax.axis_size("node")
    line = chips // PAIR
    rows, width = tokens.shape
    inner = down_weight.shape[1]
    planes = (6 * line + 3 * PAIR) * rows * width * 2 + 6 * inner * width * 2 * 1.1
    args = (tokens, expert_ids, gate_weights, gate_up_weight, down_weight)
    fits = planes < 0.9 * VMEM_BYTES and gate_up_weight.shape[0] == 1
    fits = fits and 2 * chips * cores <= LANES and pieces_of(width) > 1
    fits = fits and rows % (16 * HALVES) == 0 and line * HALVES < 12
    paired = cores == 2 and lax.axis_size("groups") * PAIR == 4
    if fits and paired and chips % PAIR == 0 and 1 < line < 9:
        return on_grid(line, *args)
    return spread_out(*args)


def solution(mesh):
    placed = (
        P(("groups", "ep", "node"), None),
        P(("groups", "ep", "node"), None),
        P(("groups", "ep", "node"), None),
        P(("ep", "node"), None, None),
        P(("ep", "node"), None, None),
    )
    return jax.shard_map(
        on_device,
        mesh=mesh,
        in_specs=placed,
        out_specs=P(("groups", "ep", "node"), None),
        check_vma=False,
    )
```
